256 devices in a mesh: rep: 16 (over z_lo, y, core), shard: 16 (over x, z_hi).
Axes of the slice: x: 4, y: 4, z: 8 (z_hi: 4, z_lo: 2; z = z_hi * 2 + z_lo), core: 2. Of those that a mesh axis runs over, the one named last changes fastest.
Arguments:
- hidden: bfloat16 [114688, 3584], P(('rep', 'shard')), may hold values from -144 to 144
- cotangent: bfloat16 [114688, 1024], P(('rep', 'shard')), may hold values from -6 to 6
- seq_ids: int32 [256, 448], P(('rep', 'shard')), may hold values from 0 to 3, as said below
- response_mask: int32 [256, 448], P(('rep', 'shard')), may hold values from 0 to 1, as said below
- group_ids: int32 [256, 4], P(('rep', 'shard')), may hold values from 0 to 127
- rewards: float32 [256, 4], P(('rep', 'shard')), may hold values from -6 to 6
- new_logp: float32 [256, 448], P(('rep', 'shard')), may hold values from -1.5 to -0.1
- old_logp: float32 [256, 448], P(('rep', 'shard')), may hold values from -1.5 to -0.1
- ref_logp: float32 [256, 448], P(('rep', 'shard')), may hold values from -1.5 to -0.1
- master: float32 [3, 3584, 1024], P(None, 'shard'), may hold values from -6 to 6
Outputs:
- new_master: float32 [3584, 1024], P('shard')
- rollout: bfloat16 [3, 3584, 4096], P(None, None, 'shard')
The draws below stay inside these ranges and needn't reach their ends.
Inputs may be any that keep to these rules, and one draw needn't show every extreme that they name: `seq_ids`: each row numbers its device's 4 sequences in token order, never falling, each with one token or more. `response_mask`: within a sequence, prompt tokens come before response tokens; a sequence may have no response tokens.
All inputs are finite; a program needn't handle non-finite values.
Results may differ from the reference program's by a relative error of at most 0.0095.
Values may be sent and summed in bfloat16 or wider, within the bound.
No kernel may reach another device: no remote copies, remote signals or barrier semaphores. Data moves between devices by JAX's collectives and lax.ppermute only.
A program may use at most 128 MiB of HBM per device.

```python
import jax
import jax.numpy as jnp
from jax import lax

D = 3584
HEAD = 128
KV_HEADS = 4
KV = 1024
TP = 8
LAYERS = 3
TOK_DEV = 448
SEQ_DEV = 4
TOKENS = 114688
GROUPS = 128
COPIES = 2
DEVICES = 256


def draw_hidden(key, part):
    column = jnp.arange(D, dtype=jnp.int32).astype(jnp.float32) / (D - 1)
    noise_key = jax.random.fold_in(key, 21)
    base = jnp.clip(jax.random.normal(noise_key, (TOKENS, D), jnp.float32), -6.0, 6.0)
    scale = 1.0 + 5.0 * column
    paired = jax.random.permutation(jax.random.fold_in(key, 22), DEVICES).astype(jnp.int32)
    row_block = jnp.arange(TOKENS, dtype=jnp.int32) // TOK_DEV
    col_block = jnp.arange(D, dtype=jnp.int32) // (D // DEVICES)
    target = paired[row_block]
    spike = jnp.where(target[:, None] == col_block[None, :], 4.0, 1.0)
    return (base * scale[None, :] * spike).astype(jnp.bfloat16)


def sequence_layout(key):
    row_keys = jax.random.split(jax.random.fold_in(key, 11), DEVICES)

    def row_bounds(row_key):
        picked = jax.random.permutation(row_key, TOK_DEV - 1)[:SEQ_DEV - 1] + 1
        return jnp.sort(picked).astype(jnp.int32)
    boundaries = jax.vmap(row_bounds)(row_keys)
    positions = jnp.arange(TOK_DEV, dtype=jnp.int32)
    seq_index = jnp.sum((positions[None, :, None] >= boundaries[:, None, :]).astype(jnp.int32), axis=2).astype(jnp.int32)
    starts = jnp.concatenate([jnp.zeros((DEVICES, 1), jnp.int32), boundaries], axis=1)
    finish = jnp.concatenate([boundaries, jnp.full((DEVICES, 1), TOK_DEV, jnp.int32)], axis=1)
    seq_lengths = finish - starts
    prompt = jax.random.randint(jax.random.fold_in(key, 12), (DEVICES, SEQ_DEV), 0, seq_lengths // 2 + 1).astype(jnp.int32)
    no_reply = jax.random.randint(jax.random.fold_in(key, 13), (DEVICES, SEQ_DEV), 0, 8) == 0
    prompt = jnp.where(no_reply, seq_lengths, prompt)
    tok_start = jnp.take_along_axis(starts, seq_index, axis=1)
    tok_prompt = jnp.take_along_axis(prompt, seq_index, axis=1)
    reply_mask = (positions[None, :] - tok_start >= tok_prompt).astype(jnp.int32)
    return (seq_index, reply_mask)


def draw_seq_ids(key, part):
    return sequence_layout(key)[0]


def draw_response_mask(key, part):
    return sequence_layout(key)[1]


def touch_ends(array, rng, low, largest):
    longest = array.shape.index(max(array.shape))
    spots = []
    for shift in (0, 1):
        where = [jax.random.randint(jax.random.fold_in(rng, axis), (), 0, length) for axis, length in enumerate(array.shape)]
        where[longest] = (where[longest] + shift) % array.shape[longest]
        spots.append(tuple(where))
    return array.at[spots[0]].set(low).at[spots[1]].set(largest)


def steps_of(own_key, dims, pieces, least, top_value):
    level, own = 1.0, jax.random.fold_in(own_key, 6)
    for position, blocks in pieces:
        heights = jnp.exp(jax.random.uniform(jax.random.fold_in(own, position), (blocks,), jnp.float32, least / len(pieces), top_value / len(pieces)))
        level = level * jnp.repeat(heights, dims[position] // blocks).reshape([-1 if axis == position else 1 for axis in range(len(dims))])
    return level


def gaussian(stream_key, shape, scale, reach, shards=(), held_as=jnp.bfloat16):
    level = steps_of(stream_key, shape, shards, -0.22, 0.18) if shards else 1.0
    values = jax.random.normal(stream_key, shape, jnp.float32) * scale * level
    return jnp.minimum(jnp.maximum(values, -reach), reach).astype(held_as)


def setup_inputs(seed: int = 0) -> dict:
    arg_keys = jax.random.split(jax.random.key(seed), 11)
    hidden = draw_hidden(jax.random.fold_in(arg_keys[10], 71), 0)
    cotangent = gaussian(arg_keys[1], (TOKENS, KV), 1.0, 6.0, ((0, 256),))
    seq_ids = draw_seq_ids(jax.random.fold_in(arg_keys[10], 71), 0)
    response_mask = draw_response_mask(jax.random.fold_in(arg_keys[10], 71), 0)
    group_ids = touch_ends(jax.random.randint(arg_keys[4], (DEVICES, SEQ_DEV), 0, GROUPS), jax.random.fold_in(arg_keys[4], 1), 0, GROUPS - 1).astype(jnp.int32)
    rewards = gaussian(arg_keys[5], (DEVICES, SEQ_DEV), 1.0, 6.0, ((0, 256),), jnp.float32)
    new_logp = jnp.clip(-1.5 + 1.4 * jax.random.uniform(arg_keys[6], (DEVICES, TOK_DEV), jnp.float32) ** steps_of(arg_keys[6], (DEVICES, TOK_DEV), ((0, 256),), -0.2, 0.2), -1.5, -0.1)
    old_logp = jnp.clip(-1.5 + 1.4 * jax.random.uniform(arg_keys[7], (DEVICES, TOK_DEV), jnp.float32) ** steps_of(arg_keys[7], (DEVICES, TOK_DEV), ((0, 256),), -0.2, 0.2), -1.5, -0.1)
    ref_logp = jnp.clip(-1.5 + 1.4 * jax.random.uniform(arg_keys[8], (DEVICES, TOK_DEV), jnp.float32) ** steps_of(arg_keys[8], (DEVICES, TOK_DEV), ((0, 256),), -0.2, 0.2), -1.5, -0.1)
    master = gaussian(arg_keys[9], (LAYERS, D, KV), 1.0, 6.0, ((1, 16),), jnp.float32)
    return dict(hidden=hidden, cotangent=cotangent, seq_ids=seq_ids, response_mask=response_mask, group_ids=group_ids, rewards=rewards, new_logp=new_logp, old_logp=old_logp, ref_logp=ref_logp, master=master)


def token_coef(seq_row, mask_row, adv_row, new_row, old_row, ref_row):
    onehot = (seq_row[:, None] == jnp.arange(SEQ_DEV, dtype=jnp.int32)[None, :]).astype(jnp.float32)
    maskf = mask_row.astype(jnp.float32)
    lengths = jnp.maximum(jnp.dot(maskf, onehot, precision=lax.Precision.HIGHEST), 1.0)
    tok_len = jnp.dot(onehot, lengths, precision=lax.Precision.HIGHEST)
    tok_adv = jnp.dot(onehot, adv_row, precision=lax.Precision.HIGHEST)
    surrogate = -tok_adv * jnp.exp(new_row - old_row) + 0.2 * (1.0 - jnp.exp(ref_row - new_row))
    return maskf / tok_len * surrogate

def group_advantage(group_flat, reward_flat, stats):
    groups = stats.shape[1]
    onehot = (group_flat[:, None] == jnp.arange(groups, dtype=jnp.int32)[None, :]).astype(jnp.float32)
    count = jnp.maximum(stats[0], 1.0)
    mean = stats[1] / count
    spread = jnp.sqrt(jnp.maximum(stats[2] / count - mean * mean, 0.0))
    tok_mean = jnp.dot(onehot, mean, precision=lax.Precision.HIGHEST)
    tok_std = jnp.dot(onehot, jnp.maximum(spread, 0.5), precision=lax.Precision.HIGHEST)
    return (reward_flat - tok_mean) / tok_std

def group_sums(group_flat, reward_flat, groups):
    onehot = (group_flat[:, None] == jnp.arange(groups, dtype=jnp.int32)[None, :]).astype(jnp.float32)
    values = jnp.stack([jnp.ones_like(reward_flat), reward_flat, reward_flat * reward_flat], axis=0)
    return jnp.dot(values, onehot, precision=lax.Precision.HIGHEST)

def device_gradient(hidden, delta):
    hidden_rows = hidden.reshape(DEVICES, TOK_DEV, D)
    delta_rows = delta.reshape(DEVICES, TOK_DEV, KV)

    def add_device(running, pair):
        term = lax.dot_general(pair[0], pair[1], (((0,), (0,)), ((), ())), preferred_element_type=jnp.float32)
        partial_value = lax.optimization_barrier(term.astype(jnp.bfloat16))
        return (running + partial_value.astype(jnp.float32), None)
    grad, _ = lax.scan(add_device, jnp.zeros((D, KV), jnp.float32), (hidden_rows, delta_rows))
    return grad

def rollout_layout(layers):
    paired = layers.reshape(LAYERS, D, 2, KV_HEADS, HEAD).transpose(0, 1, 3, 2, 4)
    paired = paired.reshape(LAYERS, D, KV_HEADS, 2 * HEAD)
    by_rank = jnp.repeat(paired, TP // KV_HEADS, axis=2)
    copies = jnp.tile(by_rank, (1, 1, COPIES, 1))
    return copies.reshape(LAYERS, D, COPIES * TP * 2 * HEAD)

def reference(hidden, cotangent, seq_ids, response_mask, group_ids, rewards, new_logp, old_logp, ref_logp, master):
    group_flat = group_ids.reshape(-1)
    reward_flat = rewards.reshape(-1)
    stats = group_sums(group_flat, reward_flat, GROUPS)
    advantage = group_advantage(group_flat, reward_flat, stats).reshape(rewards.shape)
    coef = jax.vmap(token_coef)(seq_ids, response_mask, advantage, new_logp, old_logp, ref_logp)
    delta = (coef.reshape(-1)[:, None] * cotangent.astype(jnp.float32)).astype(jnp.bfloat16)
    grad = device_gradient(hidden, delta)
    rms = jnp.sqrt(jnp.sum(grad * grad) / (D * KV) + 1e-06)
    new_master = master[0] - 0.5 * grad / rms
    layers = jnp.concatenate([new_master[None], master[1:]], axis=0).astype(jnp.bfloat16)
    rollout = rollout_layout(layers)
    return (new_master, rollout)
```

```python
import jax
import jax.numpy as jnp
from jax import lax
from jax.experimental import pallas as pl
from jax.experimental.pallas import tpu as pltpu
from jax.sharding import Mesh
from jax.sharding import PartitionSpec as P

HEAD = 128
KV_HEADS = 4
SEQ_DEV = 4
LANES = 128
REP = ("zl", "y", "c")
SHARD = ("x", "zh")
VMEM_LIMIT = 60 * 1024 * 1024
f32 = jnp.float32
bf16 = jnp.bfloat16


def swapped(value):
    return lax.ppermute(value, "c", [(0, 1), (1, 0)])


def exchanged(blocks, axis):
    return lax.all_to_all(blocks, axis, split_axis=0, concat_axis=0, tiled=True)


def sent_to_all(shard, axis):
    copies = jnp.broadcast_to(shard, (lax.axis_size(axis), *shard.shape))
    return exchanged(copies, axis)


def params(**kw):
    return pltpu.CompilerParams(vmem_limit_bytes=VMEM_LIMIT, **kw)


def cost(flops, nbytes):
    return pl.CostEstimate(flops=flops, bytes_accessed=nbytes, transcendentals=0)


def group_sums(group_flat, reward_flat, groups):
    onehot = (group_flat[:, None] == jnp.arange(groups, dtype=jnp.int32)[None, :]).astype(f32)
    values = jnp.stack([jnp.ones_like(reward_flat), reward_flat, reward_flat * reward_flat], axis=0)
    return jnp.dot(values, onehot, precision=lax.Precision.HIGHEST)


def token_rows(seq_row, mask_row, group_row, reward_row, new_row, old_row, ref_row):
    onehot = (seq_row[:, None] == jnp.arange(SEQ_DEV, dtype=jnp.int32)[None, :]).astype(f32)
    maskf = mask_row.astype(f32)
    lengths = jnp.maximum(jnp.dot(maskf, onehot, precision=lax.Precision.HIGHEST), 1.0)
    tok_len = jnp.dot(onehot, lengths, precision=lax.Precision.HIGHEST)
    tok_reward = jnp.dot(onehot, reward_row, precision=lax.Precision.HIGHEST)
    tok_group = jnp.dot(onehot, group_row.astype(f32), precision=lax.Precision.HIGHEST)
    weight = maskf / tok_len
    ratio = jnp.exp(new_row - old_row)
    penalty = 0.2 * (1.0 - jnp.exp(ref_row - new_row))
    zero = jnp.zeros_like(weight)
    return jnp.stack([weight, ratio, penalty, tok_reward, tok_group, zero, zero, zero], axis=0)


def partial_kernel(core, stats, tok_a, tok_b, cot_a, cot_b, hid_a, hid_b, out, delta_a, delta_b):
    half = cot_a.shape[1] // 2

    @pl.when(pl.program_id(0) == 0)
    def _():
        sums = jnp.sum(stats[...], axis=0)
        count = jnp.maximum(sums[0:1, :], 1.0)
        mean = sums[1:2, :] / count
        spread = jnp.maximum(jnp.sqrt(jnp.maximum(sums[2:3, :] / count - mean * mean, 0.0)), 0.5)
        cols = pl.ds(pl.multiple_of(core[0] * half, half), half)
        for tok, cot, delta in ((tok_a, cot_a, delta_a), (tok_b, cot_b, delta_b)):
            t = tok[...]
            lane = lax.broadcasted_iota(jnp.int32, (t.shape[0], LANES), 1).astype(f32)
            pick = lane == t[:, 4:5]
            tok_mean = jnp.sum(jnp.where(pick, mean, 0.0), axis=1, keepdims=True)
            tok_std = jnp.sum(jnp.where(pick, spread, 0.0), axis=1, keepdims=True)
            adv = (t[:, 3:4] - tok_mean) / tok_std
            coef = t[:, 0:1] * (-adv * t[:, 1:2] + t[:, 2:3])
            delta[...] = (coef * cot[:, cols].astype(f32)).T.astype(bf16)

    acc = jnp.dot(delta_a[...], hid_a[...], preferred_element_type=f32)
    acc = acc + jnp.dot(delta_b[...], hid_b[...], preferred_element_type=f32)
    out[...] = acc.astype(bf16).reshape(out.shape)


def partial_product(core, stats, tok_a, tok_b, cot_a, cot_b, hid_a, hid_b, nx, ny):
    toks, width = hid_a.shape
    kv = cot_a.shape[1]
    half = kv // 2
    blk = width // nx
    whole = lambda a: pl.BlockSpec(a.shape, lambda i, c: (0,) * a.ndim)
    hid = pl.BlockSpec((toks, blk), lambda i, c: (0, i))
    return pl.pallas_call(
        partial_kernel,
        out_shape=jax.ShapeDtypeStruct((nx, ny, half // ny, blk), bf16),
        grid_spec=pltpu.PrefetchScalarGridSpec(
            num_scalar_prefetch=1,
            grid=(nx,),
            in_specs=[whole(stats), whole(tok_a), whole(tok_b), whole(cot_a), whole(cot_b), hid, hid],
            out_specs=pl.BlockSpec((1, ny, half // ny, blk), lambda i, c: (i, 0, 0, 0)),
            scratch_shapes=[pltpu.VMEM((half, toks), bf16), pltpu.VMEM((half, toks), bf16)],
        ),
        compiler_params=params(),
        cost_estimate=cost(4 * toks * width * half, 4 * toks * width + 2 * width * half),
        name="partial_product",
    )(core, stats, tok_a, tok_b, cot_a, cot_b, hid_a, hid_b)


def sum_turn_kernel(src, out):
    out[...] = jnp.sum(src[...].astype(f32), axis=0).T.astype(bf16)


def sum_turn(blocks):
    n, rows, width = blocks.shape
    return pl.pallas_call(
        sum_turn_kernel,
        out_shape=jax.ShapeDtypeStruct((width, rows), bf16),
        grid=(width // LANES,),
        in_specs=[pl.BlockSpec((n, rows, LANES), lambda i: (0, 0, i))],
        out_specs=pl.BlockSpec((LANES, rows), lambda i: (i, 0)),
        compiler_params=params(),
        cost_estimate=cost(n * rows * width, 2 * n * rows * width),
        name="sum_turn",
    )(blocks)


def sum_spread_kernel(src, out):
    total = jnp.sum(src[...].astype(f32), axis=0).astype(bf16)
    for i in range(out.shape[0]):
        out[i] = total


def sum_spread(blocks, copies):
    n, rows, width = blocks.shape
    return pl.pallas_call(
        sum_spread_kernel,
        out_shape=jax.ShapeDtypeStruct((copies, rows, width), bf16),
        compiler_params=params(),
        cost_estimate=cost(n * rows * width, 4 * n * rows * width),
        name="sum_spread",
    )(blocks)


def squares_kernel(own, other, out):
    a = own[...].astype(f32)
    b = other[...].astype(f32)
    s = jnp.sum(jnp.sum(a * a + b * b, axis=0), axis=0, keepdims=True)
    s = jnp.sum(s, axis=1, keepdims=True)
    out[...] = jnp.broadcast_to(s.reshape(1, 1, 1), out.shape)


def squares_of(own, other, copies):
    return pl.pallas_call(
        squares_kernel,
        out_shape=jax.ShapeDtypeStruct((copies, 1, LANES), f32),
        compiler_params=params(),
        cost_estimate=cost(4 * own.size, 4 * own.size),
        name="squares_of",
    )(own, other)


def update_kernel(entries, core, squares, own, other, master, new, blocks):
    zl, ny, rows, width = own.shape
    total = jnp.sum(jnp.sum(squares[...], axis=0), axis=1, keepdims=True) / LANES
    rms = jnp.sqrt(total / entries + 1e-06)
    mine = core[0] == 0
    for kv in range(2):
        for y in range(ny):
            for z in range(zl):
                a, b = own[z, y], other[z, y]
                grad = (jnp.where(mine, a, b) if kv == 0 else jnp.where(mine, b, a)).astype(f32)
                r = slice(z * rows, (z + 1) * rows)
                c = slice((kv * ny + y) * width, (kv * ny + y + 1) * width)
                new[r, c] = master[0, r, c] - 0.5 * grad / rms
    sent = pl.ds(pl.multiple_of(core[0] * rows, rows), rows)
    for h in range(KV_HEADS):
        for kv in range(2):
            c = slice((kv * KV_HEADS + h) * HEAD, (kv * KV_HEADS + h + 1) * HEAD)
            value = new[sent, c].astype(bf16)
            for i in range(2):
                for j in range(2):
                    blocks[i, h, j, :, kv * HEAD : (kv + 1) * HEAD] = value


def update(core, squares, own, other, master, entries):
    _, rows, kv = master.shape
    return pl.pallas_call(
        lambda *refs: update_kernel(entries, *refs),
        out_shape=(
            jax.ShapeDtypeStruct((rows, kv), f32),
            jax.ShapeDtypeStruct((2, KV_HEADS, 2, rows // 2, 2 * HEAD), bf16),
        ),
        grid_spec=pltpu.PrefetchScalarGridSpec(
            num_scalar_prefetch=1,
            grid=(1,),
            in_specs=[
                pl.BlockSpec(squares.shape, lambda i, c: (0, 0, 0)),
                pl.BlockSpec(own.shape, lambda i, c: (0, 0, 0, 0)),
                pl.BlockSpec(other.shape, lambda i, c: (0, 0, 0, 0)),
                pl.BlockSpec((1, rows, kv), lambda i, c: (0, 0, 0)),
            ],
            out_specs=(
                pl.BlockSpec((rows, kv), lambda i, c: (0, 0)),
                pl.BlockSpec((2, KV_HEADS, 2, rows // 2, 2 * HEAD), lambda i, c: (0, 0, 0, 0, 0)),
            ),
        ),
        compiler_params=params(),
        cost_estimate=cost(4 * rows * kv, 12 * rows * kv),
        name="update",
    )(core, squares, own, other, master)


def rest_kernel(core, *refs):
    masters, out = refs[:-1], refs[-1]
    for l in range(2):
        for kv in range(2):
            value = masters[kv][1 + l].astype(bf16)
            for i in range(2):
                for j in range(2):
                    out[i, 0, j, l, :, kv * HEAD : (kv + 1) * HEAD] = value


def rest_blocks(core, master):
    layers, rows, kv = master.shape
    half = rows // 2
    spec = lambda k: pl.BlockSpec((layers, half, HEAD), lambda h, c: (0, c[0], k * KV_HEADS + h))
    return pl.pallas_call(
        rest_kernel,
        out_shape=jax.ShapeDtypeStruct((2, KV_HEADS, 2, layers - 1, half, 2 * HEAD), bf16),
        grid_spec=pltpu.PrefetchScalarGridSpec(
            num_scalar_prefetch=1,
            grid=(KV_HEADS,),
            in_specs=[spec(0), spec(1)],
            out_specs=pl.BlockSpec((2, 1, 2, layers - 1, half, 2 * HEAD), lambda h, c: (0, h, 0, 0, 0, 0)),
        ),
        compiler_params=params(),
        cost_estimate=cost(layers * rows * kv, 16 * rows * kv),
        name="rest_blocks",
    )(core, master, master)


def place_kernel(core, own, other, *refs):
    out = refs[-1]

    @pl.when(pl.program_id(2) == 0)
    def _():
        out[0, :, 0] = own[:, 0]

    @pl.when(pl.program_id(2) == 1)
    def _():
        out[0, :, 0] = other[:, 0]


def place(core, own, other, first, layers, into=None):
    n, count, half, width = own.shape
    group = n // 2
    src = pl.BlockSpec((group, 1, half, width), lambda l, s, w, c: (s, l, 0, 0))
    specs = [src, src]
    args = [core, own, other]
    alias = {}
    if into is not None:
        specs.append(pl.BlockSpec(memory_space=pl.ANY))
        args.append(into)
        alias = {3: 0}
    return pl.pallas_call(
        place_kernel,
        out_shape=jax.ShapeDtypeStruct((layers, n, 2, half, width), bf16),
        grid_spec=pltpu.PrefetchScalarGridSpec(
            num_scalar_prefetch=1,
            grid=(count, 2, 2),
            in_specs=specs,
            out_specs=pl.BlockSpec(
                (1, group, 1, half, width), lambda l, s, w, c: (first + l, s, (c[0] + w) % 2, 0, 0)
            ),
        ),
        input_output_aliases=alias,
        compiler_params=params(),
        cost_estimate=cost(own.size, 8 * own.size),
        name="place",
    )(*args)


def per_device(
    hidden,
    cotangent,
    seq_ids,
    response_mask,
    group_ids,
    rewards,
    new_logp,
    old_logp,
    ref_logp,
    master,
):
    n_x, n_y, n_z = lax.axis_size("x"), lax.axis_size("y"), lax.axis_size(("zh", "zl"))
    n_shard = lax.axis_size(SHARD)
    groups = lax.axis_size(REP) * n_shard * SEQ_DEV // 8
    layers, rows, kv = master.shape
    core = lax.axis_index("c").astype(jnp.int32).reshape(1)

    local_sums = group_sums(group_ids[0], rewards[0], groups)
    stats = sent_to_all(local_sums, REP).sum(axis=0)
    stats = sent_to_all(stats, SHARD)

    hidden_b = swapped(hidden)
    cotangent_b = swapped(cotangent)
    tok = token_rows(
        seq_ids[0], response_mask[0], group_ids[0], rewards[0], new_logp[0], old_logp[0], ref_logp[0]
    )
    tok_b = swapped(tok)

    sent = partial_product(
        core, stats, tok.T, tok_b.T, cotangent, cotangent_b, hidden, hidden_b, n_x, n_y
    )
    sent = sent.reshape(n_x * n_y, *sent.shape[2:])
    part = sum_turn(exchanged(sent, ("x", "y")))
    part = part.reshape(n_z, part.shape[0] // n_z, part.shape[1])
    zl = lax.axis_size("zl")
    own = exchanged(sum_spread(exchanged(part, ("zh", "zl")), zl * n_y), ("zl", "y"))
    other = swapped(own)
    squares = exchanged(squares_of(own, other, n_shard), SHARD)
    own = own.reshape(zl, n_y, *own.shape[1:])
    other = other.reshape(own.shape)
    new_master, first = update(core, squares, own, other, master, hidden.shape[1] * kv)

    rest = rest_blocks(core, master).reshape(n_shard, layers - 1, rows // 2, 2 * HEAD)
    rest = exchanged(rest, SHARD)
    out = place(core, rest, swapped(rest), 1, layers)
    first = exchanged(first.reshape(n_shard, 1, rows // 2, 2 * HEAD), SHARD)
    out = place(core, first, swapped(first), 0, layers, out)
    return (new_master, out.reshape(layers, n_shard * rows, 2 * HEAD))


def solution(mesh):
    split = Mesh(mesh.devices.reshape(2, 4, 2, 4, 4), REP + SHARD)
    row = P(REP + SHARD, None)
    return jax.shard_map(
        per_device,
        mesh=split,
        in_specs=(row,) * 9 + (P(None, SHARD, None),),
        out_specs=(P(SHARD, None), P(None, None, SHARD)),
        check_vma=False,
    )
```

```python
import jax
import jax.numpy as jnp
from jax import lax
from jax.experimental import pallas as pl
from jax.experimental.pallas import tpu as pltpu
from jax.sharding import Mesh
from jax.sharding import PartitionSpec as P

HEAD = 128
KV_HEADS = 4
SEQ_DEV = 4
LANES = 128
REP = ("zl", "y", "c")
SHARD = ("x", "zh")
VMEM_LIMIT = 24 * 1024 * 1024
f32 = jnp.float32
bf16 = jnp.bfloat16


def swapped(value):
    return lax.ppermute(value, "c", [(0, 1), (1, 0)])


def shifted(value, axis, by):
    n = lax.axis_size(axis)
    return lax.ppermute(value, axis, [(i, (i + by) % n) for i in range(n)])


def exchanged(blocks, axis):
    return lax.all_to_all(blocks, axis, split_axis=0, concat_axis=0, tiled=True)


def sent_to_all(shard, axis):
    copies = jnp.broadcast_to(shard, (lax.axis_size(axis), *shard.shape))
    return exchanged(copies, axis)


def params(**kw):
    return pltpu.CompilerParams(vmem_limit_bytes=VMEM_LIMIT, **kw)


def cost(flops, nbytes):
    return pl.CostEstimate(flops=flops, bytes_accessed=nbytes, transcendentals=0)


def group_sums(group_flat, reward_flat, groups):
    onehot = (group_flat[:, None] == jnp.arange(groups, dtype=jnp.int32)[None, :]).astype(f32)
    values = jnp.stack([jnp.ones_like(reward_flat), reward_flat, reward_flat * reward_flat], axis=0)
    return jnp.dot(values, onehot, precision=lax.Precision.HIGHEST)


def token_rows(seq_row, mask_row, group_row, reward_row, new_row, old_row, ref_row):
    onehot = (seq_row[:, None] == jnp.arange(SEQ_DEV, dtype=jnp.int32)[None, :]).astype(f32)
    maskf = mask_row.astype(f32)
    lengths = jnp.maximum(jnp.dot(maskf, onehot, precision=lax.Precision.HIGHEST), 1.0)
    tok_len = jnp.dot(onehot, lengths, precision=lax.Precision.HIGHEST)
    tok_reward = jnp.dot(onehot, reward_row, precision=lax.Precision.HIGHEST)
    tok_group = jnp.dot(onehot, group_row.astype(f32), precision=lax.Precision.HIGHEST)
    weight = maskf / tok_len
    ratio = jnp.exp(new_row - old_row)
    penalty = 0.2 * (1.0 - jnp.exp(ref_row - new_row))
    zero = jnp.zeros_like(weight)
    return jnp.stack([weight, ratio, penalty, tok_reward, tok_group, zero, zero, zero], axis=0)


def partial_kernel(core, stats, tok_a, tok_b, cot_a, cot_b, hid_a, hid_b, after, out, delta_a, delta_b):
    half = cot_a.shape[1] // 2

    @pl.when(pl.program_id(0) == 0)
    def _():
        sums = jnp.sum(stats[...], axis=0)
        count = jnp.maximum(sums[0:1, :], 1.0)
        mean = sums[1:2, :] / count
        spread = jnp.maximum(jnp.sqrt(jnp.maximum(sums[2:3, :] / count - mean * mean, 0.0)), 0.5)
        cols = pl.ds(pl.multiple_of(core[0] * half, half), half)
        for tok, cot, delta in ((tok_a, cot_a, delta_a), (tok_b, cot_b, delta_b)):
            t = tok[...]
            lane = lax.broadcasted_iota(jnp.int32, (t.shape[0], LANES), 1).astype(f32)
            pick = lane == t[:, 4:5]
            tok_mean = jnp.sum(jnp.where(pick, mean, 0.0), axis=1, keepdims=True)
            tok_std = jnp.sum(jnp.where(pick, spread, 0.0), axis=1, keepdims=True)
            adv = (t[:, 3:4] - tok_mean) / tok_std
            coef = t[:, 0:1] * (-adv * t[:, 1:2] + t[:, 2:3])
            delta[...] = (coef * cot[:, cols].astype(f32)).T.astype(bf16)

    acc = jnp.dot(delta_a[...], hid_a[...], preferred_element_type=f32)
    acc = acc + jnp.dot(delta_b[...], hid_b[...], preferred_element_type=f32)
    out[...] = acc.astype(bf16).reshape(out.shape)


def partial_product(core, stats, tok_a, tok_b, cot_a, cot_b, hid_a, hid_b, after, nx, ny):
    toks, width = hid_a.shape
    kv = cot_a.shape[1]
    half = kv // 2
    blk = width // nx
    whole = lambda a: pl.BlockSpec(a.shape, lambda i, c: (0,) * a.ndim)
    hid = pl.BlockSpec((toks, blk), lambda i, c: (0, i))
    return pl.pallas_call(
        partial_kernel,
        out_shape=jax.ShapeDtypeStruct((nx, ny, half // ny, blk), bf16),
        grid_spec=pltpu.PrefetchScalarGridSpec(
            num_scalar_prefetch=1,
            grid=(nx,),
            in_specs=[whole(stats), whole(tok_a), whole(tok_b), whole(cot_a), whole(cot_b), hid, hid, pl.BlockSpec(memory_space=pl.ANY)],
            out_specs=pl.BlockSpec((1, ny, half // ny, blk), lambda i, c: (i, 0, 0, 0)),
            scratch_shapes=[pltpu.VMEM((half, toks), bf16), pltpu.VMEM((half, toks), bf16)],
        ),
        compiler_params=params(),
        cost_estimate=cost(4 * toks * width * half, 4 * toks * width + 2 * width * half),
        name="partial_product",
    )(core, stats, tok_a, tok_b, cot_a, cot_b, hid_a, hid_b, after)


def sum_turn_kernel(src, out, acc):
    step = pl.program_id(0)
    total = jnp.sum(src[...].astype(f32), axis=0)

    @pl.when(step == 0)
    def _():
        acc[...] = total

    @pl.when(step > 0)
    def _():
        acc[...] += total

    @pl.when(step == pl.num_programs(0) - 1)
    def _():
        out[...] = acc[...].T.astype(bf16)


def sum_turn(blocks):
    n, rows, width = blocks.shape
    return pl.pallas_call(
        sum_turn_kernel,
        out_shape=jax.ShapeDtypeStruct((width, rows), bf16),
        grid=(4,),
        in_specs=[pl.BlockSpec((n // 4, rows, width), lambda i: (i, 0, 0))],
        out_specs=pl.BlockSpec((width, rows), lambda i: (0, 0)),
        scratch_shapes=[pltpu.VMEM((rows, width), f32)],
        compiler_params=params(),
        cost_estimate=cost(n * rows * width, 2 * n * rows * width),
        name="sum_turn",
    )(blocks)


def sum_spread_kernel(src, out):
    total = jnp.sum(src[...].astype(f32), axis=0).astype(bf16)
    for i in range(out.shape[0]):
        out[i] = total


def sum_spread(blocks, copies):
    n, rows, width = blocks.shape
    return pl.pallas_call(
        sum_spread_kernel,
        out_shape=jax.ShapeDtypeStruct((copies, rows, width), bf16),
        compiler_params=params(),
        cost_estimate=cost(n * rows * width, 4 * n * rows * width),
        name="sum_spread",
    )(blocks)


def squares_kernel(grad, out):
    g = grad[...].astype(f32)
    s = jnp.sum(jnp.sum(g * g, axis=0), axis=0, keepdims=True)
    s = jnp.sum(s, axis=1, keepdims=True)
    out[...] = jnp.broadcast_to(s.reshape(1, 1, 1), out.shape)


def squares_of(grad, copies):
    return pl.pallas_call(
        squares_kernel,
        out_shape=jax.ShapeDtypeStruct((copies, 1, LANES), f32),
        compiler_params=params(),
        cost_estimate=cost(2 * grad.size, 2 * grad.size),
        name="squares_of",
    )(grad)


def update_kernel(entries, core, squares, grad, master, new, blocks):
    zl, ny, _, rows, width = grad.shape
    total = jnp.sum(jnp.sum(squares[...], axis=0), axis=1, keepdims=True) / LANES
    rms = jnp.sqrt(total / entries + 1e-06)
    for kv in range(2):
        for y in range(ny):
            for z in range(zl):
                r = slice(z * rows, (z + 1) * rows)
                c = slice((kv * ny + y) * width, (kv * ny + y + 1) * width)
                new[r, c] = master[0, r, c] - 0.5 * grad[z, y, kv].astype(f32) / rms
    sent = pl.ds(pl.multiple_of(core[0] * rows, rows), rows)
    for h in range(KV_HEADS):
        for kv in range(2):
            c = slice((kv * KV_HEADS + h) * HEAD, (kv * KV_HEADS + h + 1) * HEAD)
            value = new[sent, c].astype(bf16)
            for i in range(2):
                for j in range(2):
                    blocks[i, h, j, :, kv * HEAD : (kv + 1) * HEAD] = value


def update(core, squares, grad, master, entries):
    _, rows, kv = master.shape
    return pl.pallas_call(
        lambda *refs: update_kernel(entries, *refs),
        out_shape=(
            jax.ShapeDtypeStruct((rows, kv), f32),
            jax.ShapeDtypeStruct((2, KV_HEADS, 2, rows // 2, 2 * HEAD), bf16),
        ),
        grid_spec=pltpu.PrefetchScalarGridSpec(
            num_scalar_prefetch=1,
            grid=(1,),
            in_specs=[
                pl.BlockSpec(squares.shape, lambda i, c: (0, 0, 0)),
                pl.BlockSpec(grad.shape, lambda i, c: (0, 0, 0, 0, 0)),
                pl.BlockSpec((1, rows, kv), lambda i, c: (0, 0, 0)),
            ],
            out_specs=(
                pl.BlockSpec((rows, kv), lambda i, c: (0, 0)),
                pl.BlockSpec((2, KV_HEADS, 2, rows // 2, 2 * HEAD), lambda i, c: (0, 0, 0, 0, 0)),
            ),
        ),
        compiler_params=params(),
        cost_estimate=cost(4 * rows * kv, 12 * rows * kv),
        name="update",
    )(core, squares, grad, master)


def rest_kernel(pos, after, *refs):
    masters, outs = refs[:8], refs[8:]
    for d in range(4):
        for l in range(2):
            for kv in range(2):
                outs[d][0, l, :, kv * HEAD : (kv + 1) * HEAD] = masters[2 * d + kv][1 + l].astype(bf16)


def rest_blocks(pos, master, after):
    layers, rows, kv = master.shape
    half = rows // 2

    def spec(d, k):
        return pl.BlockSpec(
            (layers, half, HEAD),
            lambda xl, p: (0, p[0], k * KV_HEADS + xl * 2 + ((p[2] + d) % 4) // 2),
        )

    shape = (2, layers - 1, half, 2 * HEAD)
    return pl.pallas_call(
        rest_kernel,
        out_shape=[jax.ShapeDtypeStruct(shape, bf16)] * 4,
        grid_spec=pltpu.PrefetchScalarGridSpec(
            num_scalar_prefetch=1,
            grid=(2,),
            in_specs=[pl.BlockSpec(memory_space=pl.ANY)] + [spec(d, k) for d in range(4) for k in range(2)],
            out_specs=[pl.BlockSpec((1, *shape[1:]), lambda xl, p: (xl, 0, 0, 0))] * 4,
        ),
        compiler_params=params(),
        cost_estimate=cost(layers * rows * kv, 12 * rows * kv),
        name="rest_blocks",
    )(pos, after, *([master] * 8))


def regroup_kernel(pos, after, *refs):
    parts, (same, cross) = refs[:4], refs[4:]
    xl = pos[1] % 2
    for d in range(4):
        same[d] = parts[d][xl]
        cross[d] = parts[d][1 - xl]


def regroup(pos, parts, after):
    shape = (4, *parts[0].shape[1:])
    whole = lambda s: pl.BlockSpec(s, lambda i, p: (0,) * len(s))
    return pl.pallas_call(
        regroup_kernel,
        out_shape=[jax.ShapeDtypeStruct(shape, bf16)] * 2,
        grid_spec=pltpu.PrefetchScalarGridSpec(
            num_scalar_prefetch=1,
            grid=(1,),
            in_specs=[pl.BlockSpec(memory_space=pl.ANY)] + [whole(parts[0].shape)] * 4,
            out_specs=[whole(shape)] * 2,
        ),
        compiler_params=params(),
        cost_estimate=cost(parts[0].size, 16 * parts[0].size),
        name="regroup",
    )(pos, after, *parts)


def place_rest_kernel(pos, *refs):
    srcs, out = refs[:8], refs[8]
    zh = pos[2]
    for w in range(2):
        for dx in range(4):

            @pl.when((pl.program_id(1) == dx) & (pl.program_id(2) == w))
            def _():
                for dz in range(4):
                    out[0, 0, (zh - dz + 4) % 4, 0] = srcs[4 * w + dx][dz, 0]


def place_rest(pos, own, other, layers):
    _, count, half, width = own[0].shape
    src = pl.BlockSpec((4, 1, half, width), lambda l, d, w, p: (0, l, 0, 0))
    return pl.pallas_call(
        place_rest_kernel,
        out_shape=jax.ShapeDtypeStruct((layers, 4, 4, 2, half, width), bf16),
        grid_spec=pltpu.PrefetchScalarGridSpec(
            num_scalar_prefetch=1,
            grid=(count, 4, 2),
            in_specs=[src] * 8,
            out_specs=pl.BlockSpec(
                (1, 1, 4, 1, half, width),
                lambda l, d, w, p: (1 + l, (p[1] - d + 4) % 4, 0, (p[0] + w) % 2, 0, 0),
            ),
        ),
        compiler_params=params(),
        cost_estimate=cost(own[0].size, 32 * own[0].size),
        name="place_rest",
    )(pos, *own, *other)


def place_first_kernel(pos, own, other, into, out):
    @pl.when(pl.program_id(1) == 0)
    def _():
        out[0, :, 0] = own[...]

    @pl.when(pl.program_id(1) == 1)
    def _():
        out[0, :, 0] = other[...]


def place_first(pos, own, other, into):
    n, half, width = own.shape
    group = n // 2
    src = pl.BlockSpec((group, half, width), lambda s, w, p: (s, 0, 0))
    return pl.pallas_call(
        place_first_kernel,
        out_shape=jax.ShapeDtypeStruct(into.shape, bf16),
        grid_spec=pltpu.PrefetchScalarGridSpec(
            num_scalar_prefetch=1,
            grid=(2, 2),
            in_specs=[src, src, pl.BlockSpec(memory_space=pl.ANY)],
            out_specs=pl.BlockSpec((1, group, 1, half, width), lambda s, w, p: (0, s, (p[0] + w) % 2, 0, 0)),
        ),
        input_output_aliases={3: 0},
        compiler_params=params(),
        cost_estimate=cost(own.size, 8 * own.size),
        name="place_first",
    )(pos, own, other, into)


def per_device(
    hidden,
    cotangent,
    seq_ids,
    response_mask,
    group_ids,
    rewards,
    new_logp,
    old_logp,
    ref_logp,
    master,
):
    n_x, n_y, n_z = lax.axis_size("x"), lax.axis_size("y"), lax.axis_size(("zh", "zl"))
    n_shard = lax.axis_size(SHARD)
    groups = lax.axis_size(REP) * n_shard * SEQ_DEV // 8
    layers, rows, kv = master.shape
    pos = jnp.stack([lax.axis_index(a).astype(jnp.int32) for a in ("c", "x", "zh")])

    local_sums = group_sums(group_ids[0], rewards[0], groups)
    stats = sent_to_all(local_sums, REP).sum(axis=0)
    parts = rest_blocks(pos, master, stats)
    stats = sent_to_all(stats, SHARD)
    parts = [parts[0]] + [shifted(parts[d], "zh", d) for d in range(1, 4)]

    hidden_b = swapped(hidden)
    cotangent_b = swapped(cotangent)
    tok = token_rows(
        seq_ids[0], response_mask[0], group_ids[0], rewards[0], new_logp[0], old_logp[0], ref_logp[0]
    )
    tok_b = swapped(tok)

    sent = partial_product(
        pos, stats, tok.T, tok_b.T, cotangent, cotangent_b, hidden, hidden_b, parts[0], n_x, n_y
    )
    sent = sent.reshape(n_x * n_y, *sent.shape[2:])
    part = sum_turn(exchanged(sent, ("x", "y")))
    same, cross = regroup(pos, parts, part)
    rest = [same] + [shifted(same if d % 2 == 0 else cross, "x", d) for d in range(1, 4)]
    part = part.reshape(n_z, part.shape[0] // n_z, part.shape[1])
    zl = lax.axis_size("zl")
    part = exchanged(part, ("zh", "zl"))
    grad = exchanged(sum_spread(part, zl * n_y * 2), REP)
    squares = exchanged(squares_of(grad, n_shard), SHARD)
    grad = grad.reshape(zl, n_y, 2, *grad.shape[1:])
    new_master, first = update(pos, squares, grad, master, hidden.shape[1] * kv)

    other = [swapped(r) for r in rest]
    out = place_rest(pos, rest, other, layers)
    out = out.reshape(layers, n_shard, 2, rows // 2, 2 * HEAD)
    first = exchanged(first.reshape(n_shard, rows // 2, 2 * HEAD), SHARD)
    out = place_first(pos, first, swapped(first), out)
    return (new_master, out.reshape(layers, n_shard * rows, 2 * HEAD))


def solution(mesh):
    split = Mesh(mesh.devices.reshape(2, 4, 2, 4, 4), REP + SHARD)
    row = P(REP + SHARD, None)
    return jax.shard_map(
        per_device,
        mesh=split,
        in_specs=(row,) * 9 + (P(None, SHARD, None),),
        out_specs=(P(SHARD, None), P(None, None, SHARD)),
        check_vma=False,
    )
```

```python
import jax
import jax.numpy as jnp
from jax import lax
from jax.experimental import pallas as pl
from jax.experimental.pallas import tpu as pltpu
from jax.sharding import Mesh
from jax.sharding import PartitionSpec as P

HEAD = 128
KV_HEADS = 4
SEQ_DEV = 4
LANES = 128
REP = ("zl", "y", "c")
SHARD = ("x", "zh")
VMEM_LIMIT = 24 * 1024 * 1024
f32 = jnp.float32
bf16 = jnp.bfloat16


def swapped(value):
    return lax.ppermute(value, "c", [(0, 1), (1, 0)])


def shifted(value, axis, by):
    n = lax.axis_size(axis)
    return lax.ppermute(value, axis, [(i, (i + by) % n) for i in range(n)])


def spread_out(blocks, axis):
    return [blocks[0]] + [shifted(blocks[d], axis, d) for d in range(1, 4)]


def exchanged(blocks, axis):
    return lax.all_to_all(blocks, axis, split_axis=0, concat_axis=0, tiled=True)


def sent_to_all(shard, axis):
    copies = jnp.broadcast_to(shard, (lax.axis_size(axis), *shard.shape))
    return exchanged(copies, axis)


def params(**kw):
    return pltpu.CompilerParams(vmem_limit_bytes=VMEM_LIMIT, **kw)


def cost(flops, nbytes):
    return pl.CostEstimate(flops=flops, bytes_accessed=nbytes, transcendentals=0)


def group_sums(group_flat, reward_flat, groups):
    onehot = (group_flat[:, None] == jnp.arange(groups, dtype=jnp.int32)[None, :]).astype(f32)
    values = jnp.stack([jnp.ones_like(reward_flat), reward_flat, reward_flat * reward_flat], axis=0)
    return jnp.dot(values, onehot, precision=lax.Precision.HIGHEST)


def token_rows(seq_row, mask_row, group_row, reward_row, new_row, old_row, ref_row):
    onehot = (seq_row[:, None] == jnp.arange(SEQ_DEV, dtype=jnp.int32)[None, :]).astype(f32)
    maskf = mask_row.astype(f32)
    lengths = jnp.maximum(jnp.dot(maskf, onehot, precision=lax.Precision.HIGHEST), 1.0)
    tok_len = jnp.dot(onehot, lengths, precision=lax.Precision.HIGHEST)
    tok_reward = jnp.dot(onehot, reward_row, precision=lax.Precision.HIGHEST)
    tok_group = jnp.dot(onehot, group_row.astype(f32), precision=lax.Precision.HIGHEST)
    weight = maskf / tok_len
    ratio = jnp.exp(new_row - old_row)
    penalty = 0.2 * (1.0 - jnp.exp(ref_row - new_row))
    zero = jnp.zeros_like(weight)
    return jnp.stack([weight, ratio, penalty, tok_reward, tok_group, zero, zero, zero], axis=0)


def partial_kernel(pos, stats, tok_a, tok_b, cot_a, cot_b, hid_a, hid_b, *refs):
    outs, (delta_a, delta_b) = refs[:8], refs[8:]
    half = cot_a.shape[1] // 2
    rows = outs[0].shape[1]
    step = pl.program_id(0)

    @pl.when(step == 0)
    def _():
        sums = jnp.sum(stats[...], axis=0)
        count = jnp.maximum(sums[0:1, :], 1.0)
        mean = sums[1:2, :] / count
        spread = jnp.maximum(jnp.sqrt(jnp.maximum(sums[2:3, :] / count - mean * mean, 0.0)), 0.5)
        cols = pl.ds(pl.multiple_of(pos[0] * half, half), half)
        for tok, cot, delta in ((tok_a, cot_a, delta_a), (tok_b, cot_b, delta_b)):
            t = tok[...]
            lane = lax.broadcasted_iota(jnp.int32, (t.shape[0], LANES), 1).astype(f32)
            pick = lane == t[:, 4:5]
            tok_mean = jnp.sum(jnp.where(pick, mean, 0.0), axis=1, keepdims=True)
            tok_std = jnp.sum(jnp.where(pick, spread, 0.0), axis=1, keepdims=True)
            adv = (t[:, 3:4] - tok_mean) / tok_std
            coef = t[:, 0:1] * (-adv * t[:, 1:2] + t[:, 2:3])
            turned = (coef * cot[:, cols].astype(f32)).T.astype(bf16)
            for y in range(4):
                delta[y * rows : (y + 1) * rows, :] = turned[2 * y * rows : (2 * y + 1) * rows]
                to = pl.multiple_of((4 + (y - pos[3] + 4) % 4) * rows, rows)
                delta[pl.ds(to, rows), :] = turned[(2 * y + 1) * rows : (2 * y + 2) * rows]

    acc = jnp.dot(delta_a[...], hid_a[...], preferred_element_type=f32)
    acc = acc + jnp.dot(delta_b[...], hid_b[...], preferred_element_type=f32)
    acc = acc.astype(bf16).reshape(8, rows, acc.shape[1])
    for d in range(4):

        @pl.when(step == d)
        def _():
            outs[d][...] = acc[:4]

        outs[4 + d][(pos[1] + step) % 4] = acc[4 + d]


def partial_product(pos, stats, tok_a, tok_b, cot_a, cot_b, hid_a, hid_b):
    toks, width = hid_a.shape
    half = cot_a.shape[1] // 2
    blk = width // 4
    shape = (4, half // 8, blk)
    whole = lambda a: pl.BlockSpec(a.shape, lambda i, p: (0,) * a.ndim)
    hid = pl.BlockSpec((toks, blk), lambda i, p: (0, (p[1] + i) % 4))
    return pl.pallas_call(
        partial_kernel,
        out_shape=[jax.ShapeDtypeStruct(shape, bf16)] * 8,
        grid_spec=pltpu.PrefetchScalarGridSpec(
            num_scalar_prefetch=1,
            grid=(4,),
            in_specs=[whole(stats), whole(tok_a), whole(tok_b), whole(cot_a), whole(cot_b), hid, hid],
            out_specs=[pl.BlockSpec(shape, lambda i, p: (0, 0, 0))] * 8,
            scratch_shapes=[pltpu.VMEM((half, toks), bf16), pltpu.VMEM((half, toks), bf16)],
        ),
        compiler_params=params(),
        cost_estimate=cost(4 * toks * width * half, 4 * toks * width + 2 * width * half),
        name="partial_product",
    )(pos, stats, tok_a, tok_b, cot_a, cot_b, hid_a, hid_b)


def sum_mid_kernel(pos, *refs):
    for half in range(2):
        srcs, outs = refs[4 * half : 4 * half + 4], refs[8 + 4 * half : 12 + 4 * half]
        at = pos[3] if half == 0 else pos[1]
        for d in range(4):
            k = (at + d) % 4
            outs[d][...] = sum(src[k].astype(f32) for src in srcs).astype(bf16)


def sum_mid(pos, first, second):
    _, rows, width = first[0].shape
    whole = lambda *shape: pl.BlockSpec(shape, lambda i, p: (0,) * len(shape))
    out = pl.pallas_call(
        sum_mid_kernel,
        out_shape=[jax.ShapeDtypeStruct((rows, width), bf16)] * 8,
        grid_spec=pltpu.PrefetchScalarGridSpec(
            num_scalar_prefetch=1,
            grid=(1,),
            in_specs=[whole(4, rows, width)] * 8,
            out_specs=[whole(rows, width)] * 8,
        ),
        compiler_params=params(),
        cost_estimate=cost(32 * rows * width, 80 * rows * width),
        name="sum_mid",
    )(pos, *first, *second)
    return out[:4], out[4:]


def sum_turn_kernel(*refs):
    srcs, out = refs[:8], refs[8]
    first = sum(src[...].astype(f32) for src in srcs[:4])
    second = sum(src[...].astype(f32) for src in srcs[4:])
    out[...] = jnp.concatenate([first, second], axis=0).T.astype(bf16)


def sum_turn(first, second):
    rows, width = first[0].shape
    return pl.pallas_call(
        sum_turn_kernel,
        out_shape=jax.ShapeDtypeStruct((width, 2 * rows), bf16),
        compiler_params=params(),
        cost_estimate=cost(8 * rows * width, 20 * rows * width),
        name="sum_turn",
    )(*first, *second)


def sum_spread_kernel(src, out):
    total = jnp.sum(src[...].astype(f32), axis=0).astype(bf16)
    for i in range(out.shape[0]):
        out[i] = total


def sum_spread(blocks, copies):
    n, rows, width = blocks.shape
    return pl.pallas_call(
        sum_spread_kernel,
        out_shape=jax.ShapeDtypeStruct((copies, rows, width), bf16),
        compiler_params=params(),
        cost_estimate=cost(n * rows * width, 4 * n * rows * width),
        name="sum_spread",
    )(blocks)


def squares_kernel(grad, out):
    g = grad[...].astype(f32)
    s = jnp.sum(jnp.sum(g * g, axis=0), axis=0, keepdims=True)
    s = jnp.sum(s, axis=1, keepdims=True)
    out[...] = jnp.broadcast_to(s.reshape(1, 1, 1), out.shape)


def squares_of(grad, copies):
    return pl.pallas_call(
        squares_kernel,
        out_shape=jax.ShapeDtypeStruct((copies, 1, LANES), f32),
        compiler_params=params(),
        cost_estimate=cost(2 * grad.size, 2 * grad.size),
        name="squares_of",
    )(grad)


def update_kernel(entries, core, squares, grad, master, new, blocks):
    zl, ny, _, rows, width = grad.shape
    total = jnp.sum(jnp.sum(squares[...], axis=0), axis=1, keepdims=True) / LANES
    rms = jnp.sqrt(total / entries + 1e-06)
    for kv in range(2):
        for y in range(ny):
            for z in range(zl):
                r = slice(z * rows, (z + 1) * rows)
                c = slice((kv * ny + y) * width, (kv * ny + y + 1) * width)
                new[r, c] = master[0, r, c] - 0.5 * grad[z, y, kv].astype(f32) / rms
    sent = pl.ds(pl.multiple_of(core[0] * rows, rows), rows)
    for h in range(KV_HEADS):
        for kv in range(2):
            c = slice((kv * KV_HEADS + h) * HEAD, (kv * KV_HEADS + h + 1) * HEAD)
            value = new[sent, c].astype(bf16)
            for i in range(2):
                for j in range(2):
                    blocks[i, h, j, :, kv * HEAD : (kv + 1) * HEAD] = value


def update(core, squares, grad, master, entries):
    _, rows, kv = master.shape
    return pl.pallas_call(
        lambda *refs: update_kernel(entries, *refs),
        out_shape=(
            jax.ShapeDtypeStruct((rows, kv), f32),
            jax.ShapeDtypeStruct((2, KV_HEADS, 2, rows // 2, 2 * HEAD), bf16),
        ),
        grid_spec=pltpu.PrefetchScalarGridSpec(
            num_scalar_prefetch=1,
            grid=(1,),
            in_specs=[
                pl.BlockSpec(squares.shape, lambda i, c: (0, 0, 0)),
                pl.BlockSpec(grad.shape, lambda i, c: (0, 0, 0, 0, 0)),
                pl.BlockSpec((1, rows, kv), lambda i, c: (0, 0, 0)),
            ],
            out_specs=(
                pl.BlockSpec((rows, kv), lambda i, c: (0, 0)),
                pl.BlockSpec((2, KV_HEADS, 2, rows // 2, 2 * HEAD), lambda i, c: (0, 0, 0, 0, 0)),
            ),
        ),
        compiler_params=params(),
        cost_estimate=cost(4 * rows * kv, 12 * rows * kv),
        name="update",
    )(core, squares, grad, master)


def rest_kernel(pos, *refs):
    masters, outs = refs[:8], refs[8:]
    for d in range(4):
        for l in range(2):
            for kv in range(2):
                outs[d][0, l, :, kv * HEAD : (kv + 1) * HEAD] = masters[2 * d + kv][1 + l].astype(bf16)


def rest_blocks(pos, master):
    layers, rows, kv = master.shape
    half = rows // 2

    def spec(d, k):
        return pl.BlockSpec(
            (layers, half, HEAD),
            lambda xl, p: (0, p[0], k * KV_HEADS + xl * 2 + ((p[2] + d) % 4) // 2),
        )

    shape = (2, layers - 1, half, 2 * HEAD)
    return pl.pallas_call(
        rest_kernel,
        out_shape=[jax.ShapeDtypeStruct(shape, bf16)] * 4,
        grid_spec=pltpu.PrefetchScalarGridSpec(
            num_scalar_prefetch=1,
            grid=(2,),
            in_specs=[spec(d, k) for d in range(4) for k in range(2)],
            out_specs=[pl.BlockSpec((1, *shape[1:]), lambda xl, p: (xl, 0, 0, 0))] * 4,
        ),
        compiler_params=params(),
        cost_estimate=cost(layers * rows * kv, 12 * rows * kv),
        name="rest_blocks",
    )(pos, *([master] * 8))


def regroup_kernel(pos, *refs):
    parts, (same, cross) = refs[:4], refs[4:]
    xl = pos[1] % 2
    for d in range(4):
        same[d] = parts[d][xl]
        cross[d] = parts[d][1 - xl]


def regroup(pos, parts):
    shape = (4, *parts[0].shape[1:])
    whole = lambda s: pl.BlockSpec(s, lambda i, p: (0,) * len(s))
    return pl.pallas_call(
        regroup_kernel,
        out_shape=[jax.ShapeDtypeStruct(shape, bf16)] * 2,
        grid_spec=pltpu.PrefetchScalarGridSpec(
            num_scalar_prefetch=1,
            grid=(1,),
            in_specs=[whole(parts[0].shape)] * 4,
            out_specs=[whole(shape)] * 2,
        ),
        compiler_params=params(),
        cost_estimate=cost(parts[0].size, 16 * parts[0].size),
        name="regroup",
    )(pos, *parts)


def place_rest_kernel(pos, *refs):
    srcs, out = refs[:8], refs[8]
    zh = pos[2]
    for w in range(2):
        for dx in range(4):

            @pl.when((pl.program_id(1) == dx) & (pl.program_id(2) == w))
            def _():
                for dz in range(4):
                    out[0, 0, (zh - dz + 4) % 4, 0] = srcs[4 * w + dx][dz, 0]


def place_rest(pos, own, other, layers):
    _, count, half, width = own[0].shape
    src = pl.BlockSpec((4, 1, half, width), lambda l, d, w, p: (0, l, 0, 0))
    return pl.pallas_call(
        place_rest_kernel,
        out_shape=jax.ShapeDtypeStruct((layers, 4, 4, 2, half, width), bf16),
        grid_spec=pltpu.PrefetchScalarGridSpec(
            num_scalar_prefetch=1,
            grid=(count, 4, 2),
            in_specs=[src] * 8,
            out_specs=pl.BlockSpec(
                (1, 1, 4, 1, half, width),
                lambda l, d, w, p: (1 + l, (p[1] - d + 4) % 4, 0, (p[0] + w) % 2, 0, 0),
            ),
        ),
        compiler_params=params(),
        cost_estimate=cost(own[0].size, 32 * own[0].size),
        name="place_rest",
    )(pos, *own, *other)


def place_first_kernel(pos, own, other, into, out):
    @pl.when(pl.program_id(1) == 0)
    def _():
        out[0, :, 0] = own[...]

    @pl.when(pl.program_id(1) == 1)
    def _():
        out[0, :, 0] = other[...]


def place_first(pos, own, other, into):
    n, half, width = own.shape
    group = n // 2
    src = pl.BlockSpec((group, half, width), lambda s, w, p: (s, 0, 0))
    return pl.pallas_call(
        place_first_kernel,
        out_shape=jax.ShapeDtypeStruct(into.shape, bf16),
        grid_spec=pltpu.PrefetchScalarGridSpec(
            num_scalar_prefetch=1,
            grid=(2, 2),
            in_specs=[src, src, pl.BlockSpec(memory_space=pl.ANY)],
            out_specs=pl.BlockSpec((1, group, 1, half, width), lambda s, w, p: (0, s, (p[0] + w) % 2, 0, 0)),
        ),
        input_output_aliases={3: 0},
        compiler_params=params(),
        cost_estimate=cost(own.size, 8 * own.size),
        name="place_first",
    )(pos, own, other, into)


def per_device(
    hidden,
    cotangent,
    seq_ids,
    response_mask,
    group_ids,
    rewards,
    new_logp,
    old_logp,
    ref_logp,
    master,
):
    n_y, n_z = lax.axis_size("y"), lax.axis_size(("zh", "zl"))
    n_shard = lax.axis_size(SHARD)
    groups = lax.axis_size(REP) * n_shard * SEQ_DEV // 8
    layers, rows, kv = master.shape
    pos = jnp.stack([lax.axis_index(a).astype(jnp.int32) for a in ("c", "x", "zh", "y")])

    local_sums = group_sums(group_ids[0], rewards[0], groups)
    stats = sent_to_all(local_sums, REP).sum(axis=0)
    stats = sent_to_all(stats, SHARD)

    hidden_b = swapped(hidden)
    cotangent_b = swapped(cotangent)
    tok = token_rows(
        seq_ids[0], response_mask[0], group_ids[0], rewards[0], new_logp[0], old_logp[0], ref_logp[0]
    )
    tok_b = swapped(tok)

    partial = partial_product(pos, stats, tok.T, tok_b.T, cotangent, cotangent_b, hidden, hidden_b)
    to_x = spread_out(partial[:4], "x")
    to_y = spread_out(partial[4:], "y")
    to_y, to_x = sum_mid(pos, to_x, to_y)
    to_y = spread_out(to_y, "y")
    to_x = spread_out(to_x, "x")
    part = sum_turn(to_y, to_x)

    parts = rest_blocks(pos, master)
    parts = spread_out(parts, "zh")
    same, cross = regroup(pos, parts)
    rest = spread_out([same, cross, same, cross], "x")
    part = part.reshape(n_z, part.shape[0] // n_z, part.shape[1])
    zl = lax.axis_size("zl")
    part = exchanged(part, ("zh", "zl"))
    grad = exchanged(sum_spread(part, zl * n_y * 2), REP)
    squares = exchanged(squares_of(grad, n_shard), SHARD)
    grad = grad.reshape(zl, n_y, 2, *grad.shape[1:])
    new_master, first = update(pos, squares, grad, master, hidden.shape[1] * kv)

    other = [swapped(r) for r in rest]
    out = place_rest(pos, rest, other, layers)
    out = out.reshape(layers, n_shard, 2, rows // 2, 2 * HEAD)
    first = exchanged(first.reshape(n_shard, rows // 2, 2 * HEAD), SHARD)
    out = place_first(pos, first, swapped(first), out)
    return (new_master, out.reshape(layers, n_shard * rows, 2 * HEAD))


def solution(mesh):
    split = Mesh(mesh.devices.reshape(2, 4, 2, 4, 4), REP + SHARD)
    row = P(REP + SHARD, None)
    return jax.shard_map(
        per_device,
        mesh=split,
        in_specs=(row,) * 9 + (P(None, SHARD, None),),
        out_specs=(P(SHARD, None), P(None, None, SHARD)),
        check_vma=False,
    )
```

```python
import jax
import jax.numpy as jnp
from jax import lax
from jax.experimental import pallas as pl
from jax.experimental.pallas import tpu as pltpu
from jax.sharding import Mesh
from jax.sharding import PartitionSpec as P

HEAD = 128
KV_HEADS = 4
SEQ_DEV = 4
LANES = 128
REP = ("zl", "y", "c")
SHARD = ("x", "zh")
VMEM_LIMIT = 24 * 1024 * 1024
f32 = jnp.float32
bf16 = jnp.bfloat16


def swapped(value):
    return lax.ppermute(value, "c", [(0, 1), (1, 0)])


def shifted(value, axis, by):
    n = lax.axis_size(axis)
    return lax.ppermute(value, axis, [(i, (i + by) % n) for i in range(n)])


def spread_out(blocks, axis):
    return [blocks[0]] + [shifted(blocks[d], axis, d) for d in range(1, 4)]


def exchanged(blocks, axis):
    return lax.all_to_all(blocks, axis, split_axis=0, concat_axis=0, tiled=True)


def sent_to_all(shard, axis):
    copies = jnp.broadcast_to(shard, (lax.axis_size(axis), *shard.shape))
    return exchanged(copies, axis)


def params(**kw):
    return pltpu.CompilerParams(vmem_limit_bytes=VMEM_LIMIT, **kw)


def cost(flops, nbytes):
    return pl.CostEstimate(flops=flops, bytes_accessed=nbytes, transcendentals=0)


def group_sums(group_flat, reward_flat, groups):
    onehot = (group_flat[:, None] == jnp.arange(groups, dtype=jnp.int32)[None, :]).astype(f32)
    values = jnp.stack([jnp.ones_like(reward_flat), reward_flat, reward_flat * reward_flat], axis=0)
    return jnp.dot(values, onehot, precision=lax.Precision.HIGHEST)


def token_rows(seq_row, mask_row, group_row, reward_row, new_row, old_row, ref_row):
    onehot = (seq_row[:, None] == jnp.arange(SEQ_DEV, dtype=jnp.int32)[None, :]).astype(f32)
    maskf = mask_row.astype(f32)
    lengths = jnp.maximum(jnp.dot(maskf, onehot, precision=lax.Precision.HIGHEST), 1.0)
    tok_len = jnp.dot(onehot, lengths, precision=lax.Precision.HIGHEST)
    tok_reward = jnp.dot(onehot, reward_row, precision=lax.Precision.HIGHEST)
    tok_group = jnp.dot(onehot, group_row.astype(f32), precision=lax.Precision.HIGHEST)
    weight = maskf / tok_len
    ratio = jnp.exp(new_row - old_row)
    penalty = 0.2 * (1.0 - jnp.exp(ref_row - new_row))
    zero = jnp.zeros_like(weight)
    return jnp.stack([weight, ratio, penalty, tok_reward, tok_group, zero, zero, zero], axis=0)


def partial_kernel(pos, stats, tok_a, tok_b, cot_a, cot_b, hid_a, hid_b, *refs):
    outs, (delta_a, delta_b) = refs[:8], refs[8:]
    half = cot_a.shape[1] // 2
    rows = outs[0].shape[1]
    step = pl.program_id(0)

    @pl.when(step == 0)
    def _():
        sums = jnp.sum(stats[...], axis=0)
        count = jnp.maximum(sums[0:1, :], 1.0)
        mean = sums[1:2, :] / count
        spread = jnp.maximum(jnp.sqrt(jnp.maximum(sums[2:3, :] / count - mean * mean, 0.0)), 0.5)
        cols = pl.ds(pl.multiple_of(pos[0] * half, half), half)
        for tok, cot, delta in ((tok_a, cot_a, delta_a), (tok_b, cot_b, delta_b)):
            t = tok[...]
            lane = lax.broadcasted_iota(jnp.int32, (t.shape[0], LANES), 1).astype(f32)
            pick = lane == t[:, 4:5]
            tok_mean = jnp.sum(jnp.where(pick, mean, 0.0), axis=1, keepdims=True)
            tok_std = jnp.sum(jnp.where(pick, spread, 0.0), axis=1, keepdims=True)
            adv = (t[:, 3:4] - tok_mean) / tok_std
            coef = t[:, 0:1] * (-adv * t[:, 1:2] + t[:, 2:3])
            turned = (coef * cot[:, cols].astype(f32)).T.astype(bf16)
            for y in range(4):
                delta[y * rows : (y + 1) * rows, :] = turned[2 * y * rows : (2 * y + 1) * rows]
                to = pl.multiple_of((4 + (y - pos[3] + 4) % 4) * rows, rows)
                delta[pl.ds(to, rows), :] = turned[(2 * y + 1) * rows : (2 * y + 2) * rows]

    acc = jnp.dot(delta_a[...], hid_a[...], preferred_element_type=f32)
    acc = acc + jnp.dot(delta_b[...], hid_b[...], preferred_element_type=f32)
    acc = acc.astype(bf16).reshape(8, rows, acc.shape[1])
    for d in range(4):

        @pl.when(step == d)
        def _():
            outs[d][...] = acc[:4]

        outs[4 + d][(pos[1] + step) % 4] = acc[4 + d]


def partial_product(pos, stats, tok_a, tok_b, cot_a, cot_b, hid_a, hid_b):
    toks, width = hid_a.shape
    half = cot_a.shape[1] // 2
    blk = width // 4
    shape = (4, half // 8, blk)
    whole = lambda a: pl.BlockSpec(a.shape, lambda i, p: (0,) * a.ndim)
    hid = pl.BlockSpec((toks, blk), lambda i, p: (0, (p[1] + i) % 4))
    return pl.pallas_call(
        partial_kernel,
        out_shape=[jax.ShapeDtypeStruct(shape, bf16)] * 8,
        grid_spec=pltpu.PrefetchScalarGridSpec(
            num_scalar_prefetch=1,
            grid=(4,),
            in_specs=[whole(stats), whole(tok_a), whole(tok_b), whole(cot_a), whole(cot_b), hid, hid],
            out_specs=[pl.BlockSpec(shape, lambda i, p: (0, 0, 0))] * 8,
            scratch_shapes=[pltpu.VMEM((half, toks), bf16), pltpu.VMEM((half, toks), bf16)],
        ),
        compiler_params=params(),
        cost_estimate=cost(4 * toks * width * half, 4 * toks * width + 2 * width * half),
        name="partial_product",
    )(pos, stats, tok_a, tok_b, cot_a, cot_b, hid_a, hid_b)


def sum_mid_kernel(pos, *refs):
    for half in range(2):
        srcs, outs = refs[4 * half : 4 * half + 4], refs[8 + 4 * half : 12 + 4 * half]
        at = pos[3] if half == 0 else pos[1]
        for d in range(4):
            k = (at + d) % 4
            outs[d][...] = sum(src[k].astype(f32) for src in srcs).astype(bf16)


def sum_mid(pos, first, second):
    _, rows, width = first[0].shape
    whole = lambda *shape: pl.BlockSpec(shape, lambda i, p: (0,) * len(shape))
    out = pl.pallas_call(
        sum_mid_kernel,
        out_shape=[jax.ShapeDtypeStruct((rows, width), bf16)] * 8,
        grid_spec=pltpu.PrefetchScalarGridSpec(
            num_scalar_prefetch=1,
            grid=(1,),
            in_specs=[whole(4, rows, width)] * 8,
            out_specs=[whole(rows, width)] * 8,
        ),
        compiler_params=params(),
        cost_estimate=cost(32 * rows * width, 80 * rows * width),
        name="sum_mid",
    )(pos, *first, *second)
    return out[:4], out[4:]


def sum_turn_kernel(*refs):
    srcs, out = refs[:8], refs[8]
    first = sum(src[...].astype(f32) for src in srcs[:4])
    second = sum(src[...].astype(f32) for src in srcs[4:])
    out[...] = jnp.concatenate([first, second], axis=0).T.astype(bf16)


def sum_turn(first, second):
    rows, width = first[0].shape
    return pl.pallas_call(
        sum_turn_kernel,
        out_shape=jax.ShapeDtypeStruct((width, 2 * rows), bf16),
        compiler_params=params(),
        cost_estimate=cost(8 * rows * width, 20 * rows * width),
        name="sum_turn",
    )(*first, *second)


def sum_spread_kernel(src, out):
    total = jnp.sum(src[...].astype(f32), axis=0).astype(bf16)
    for i in range(out.shape[0]):
        out[i] = total


def sum_spread(blocks, copies):
    n, rows, width = blocks.shape
    return pl.pallas_call(
        sum_spread_kernel,
        out_shape=jax.ShapeDtypeStruct((copies, rows, width), bf16),
        compiler_params=params(),
        cost_estimate=cost(n * rows * width, 4 * n * rows * width),
        name="sum_spread",
    )(blocks)


def send_kernel(pos, grad, blocks):
    g = grad[...].astype(f32)
    s = jnp.sum(g * g, axis=(0, 1, 2))
    s = jnp.sum(jnp.sum(s, axis=0, keepdims=True), axis=1, keepdims=True)
    high = s.astype(bf16).astype(f32)
    mid = (s - high).astype(bf16).astype(f32)
    low = s - high - mid
    rows = grad.shape[3]
    row = lax.broadcasted_iota(jnp.int32, (8, 2 * HEAD), 0)
    tail = jnp.where(row == 0, high, jnp.where(row == 1, mid, jnp.where(row == 2, low, 0.0))).astype(bf16)
    for h in range(KV_HEADS):
        for i in range(2):
            for j in range(2):
                for kv in range(2):
                    blocks[i, h, j, :rows, kv * HEAD : (kv + 1) * HEAD] = grad[pos[0], h, kv]
                blocks[i, h, j, rows:, :] = tail


def send_blocks(pos, grad):
    rows = grad.shape[3]
    whole = lambda s: pl.BlockSpec(s, lambda i, p: (0,) * len(s))
    shape = (2, KV_HEADS, 2, rows + 8, 2 * HEAD)
    return pl.pallas_call(
        send_kernel,
        out_shape=jax.ShapeDtypeStruct(shape, bf16),
        grid_spec=pltpu.PrefetchScalarGridSpec(
            num_scalar_prefetch=1, grid=(1,), in_specs=[whole(grad.shape)], out_specs=whole(shape)
        ),
        compiler_params=params(),
        cost_estimate=cost(4 * grad.size, 8 * grad.size),
        name="send_blocks",
    )(pos, grad)


def step_size(squares, entries):
    s = jnp.sum(squares[...].astype(f32), axis=0)[:, 0:1]
    total = s[0:1] + s[1:2] + s[2:3]
    return 0.5 / jnp.sqrt(total / entries + 1e-06)


def update_kernel(entries, squares, grad, master, new):
    zl, ny, _, rows, width = grad.shape
    step = step_size(squares, entries)
    for kv in range(2):
        for y in range(ny):
            for z in range(zl):
                r = slice(z * rows, (z + 1) * rows)
                c = slice((kv * ny + y) * width, (kv * ny + y + 1) * width)
                new[r, c] = master[0, r, c] - grad[z, y, kv].astype(f32) * step


def update(received, grad, master, entries):
    _, rows, kv = master.shape
    return pl.pallas_call(
        lambda *refs: update_kernel(entries, *refs),
        out_shape=jax.ShapeDtypeStruct((rows, kv), f32),
        grid=(1,),
        in_specs=[
            pl.BlockSpec((received.shape[0], 8, LANES), lambda i: (0, rows // 16, 0)),
            pl.BlockSpec(grad.shape, lambda i: (0, 0, 0, 0, 0)),
            pl.BlockSpec((1, rows, kv), lambda i: (0, 0, 0)),
        ],
        out_specs=pl.BlockSpec((rows, kv), lambda i: (0, 0)),
        compiler_params=params(),
        cost_estimate=cost(4 * rows * kv, 10 * rows * kv),
        name="update",
    )(received, grad, master)


def rest_kernel(pos, *refs):
    masters, outs = refs[:8], refs[8:]
    for d in range(4):
        for kv in range(2):
            outs[d][0, :, :, kv * HEAD : (kv + 1) * HEAD] = masters[2 * d + kv][...].astype(bf16)


def rest_blocks(pos, master):
    layers, rows, kv = master.shape
    half = rows // 2

    def spec(d, k):
        return pl.BlockSpec(
            (layers, half, HEAD),
            lambda xl, p: (0, p[0], k * KV_HEADS + xl * 2 + ((p[2] + d) % 4) // 2),
        )

    shape = (2, layers, half, 2 * HEAD)
    return pl.pallas_call(
        rest_kernel,
        out_shape=[jax.ShapeDtypeStruct(shape, bf16)] * 4,
        grid_spec=pltpu.PrefetchScalarGridSpec(
            num_scalar_prefetch=1,
            grid=(2,),
            in_specs=[spec(d, k) for d in range(4) for k in range(2)],
            out_specs=[pl.BlockSpec((1, *shape[1:]), lambda xl, p: (xl, 0, 0, 0))] * 4,
        ),
        compiler_params=params(),
        cost_estimate=cost(layers * rows * kv, 12 * rows * kv),
        name="rest_blocks",
    )(pos, *([master] * 8))


def regroup_kernel(pos, *refs):
    parts, (same, cross), sems = refs[:4], refs[4:6], refs[6]
    xl = pos[1] % 2
    copies = []
    for d in range(4):
        copies.append(pltpu.make_async_copy(parts[d].at[xl], same.at[d], sems.at[2 * d]))
        copies.append(pltpu.make_async_copy(parts[d].at[1 - xl], cross.at[d], sems.at[2 * d + 1]))
    for copy in copies:
        copy.start()
    for copy in copies:
        copy.wait()


def regroup(pos, parts):
    shape = (4, *parts[0].shape[1:])
    whole = lambda s: pl.BlockSpec(s, lambda i, p: (0,) * len(s))
    return pl.pallas_call(
        regroup_kernel,
        out_shape=[jax.ShapeDtypeStruct(shape, bf16)] * 2,
        grid_spec=pltpu.PrefetchScalarGridSpec(
            num_scalar_prefetch=1,
            grid=(1,),
            in_specs=[pl.BlockSpec(memory_space=pltpu.HBM)] * 4,
            out_specs=[whole(shape)] * 2,
            scratch_shapes=[pltpu.SemaphoreType.DMA((8,))],
        ),
        compiler_params=params(),
        cost_estimate=cost(parts[0].size, 16 * parts[0].size),
        name="regroup",
    )(pos, *parts)


def place_rest_kernel(pos, *refs):
    srcs, out = refs[:8], refs[8]
    zh = pos[2]
    for w in range(2):
        for dx in range(4):

            @pl.when((pl.program_id(1) == dx) & (pl.program_id(2) == w))
            def _():
                for dz in range(4):
                    out[0, 0, (zh - dz + 4) % 4, 0] = srcs[4 * w + dx][dz, 0]


def place_rest(pos, own, other, layers):
    _, count, half, width = own[0].shape
    src = pl.BlockSpec((4, 1, half, width), lambda l, d, w, p: (0, 1 + l, 0, 0))
    return pl.pallas_call(
        place_rest_kernel,
        out_shape=jax.ShapeDtypeStruct((layers, 4, 4, 2, half, width), bf16),
        grid_spec=pltpu.PrefetchScalarGridSpec(
            num_scalar_prefetch=1,
            grid=(count - 1, 4, 2),
            in_specs=[src] * 8,
            out_specs=pl.BlockSpec(
                (1, 1, 4, 1, half, width),
                lambda l, d, w, p: (1 + l, (p[1] - d + 4) % 4, 0, (p[0] + w) % 2, 0, 0),
            ),
        ),
        compiler_params=params(),
        cost_estimate=cost(own[0].size, 32 * own[0].size),
        name="place_rest",
    )(pos, *own, *other)


def finish_kernel(entries, pos, squares, grad_a, grad_b, *refs):
    masters, out = refs[:8], refs[9]
    zh = pos[2]
    step = step_size(squares, entries)
    half = out.shape[4]
    for w in range(2):
        grad = (grad_a, grad_b)[w]
        for dx in range(4):

            @pl.when((pl.program_id(0) == dx) & (pl.program_id(1) == w))
            def _():
                for dz in range(4):
                    k = (zh - dz + 4) % 4
                    value = masters[4 * w + dx][dz, 0].astype(f32) - grad[k, :half].astype(f32) * step
                    out[0, 0, k, 0] = value.astype(bf16)


def finish(pos, grad_a, grad_b, own, other, into, entries):
    n, padded, width = grad_a.shape
    half = padded - 8
    grad = pl.BlockSpec((4, padded, width), lambda d, w, p: ((p[1] - d + 4) % 4, 0, 0))
    src = pl.BlockSpec((4, 1, half, width), lambda d, w, p: (0, 0, 0, 0))
    return pl.pallas_call(
        lambda *refs: finish_kernel(entries, *refs),
        out_shape=jax.ShapeDtypeStruct(into.shape, bf16),
        grid_spec=pltpu.PrefetchScalarGridSpec(
            num_scalar_prefetch=1,
            grid=(4, 2),
            in_specs=[pl.BlockSpec((n, 8, LANES), lambda d, w, p: (0, half // 8, 0)), grad, grad]
            + [src] * 8
            + [pl.BlockSpec(memory_space=pl.ANY)],
            out_specs=pl.BlockSpec(
                (1, 1, 4, 1, half, width), lambda d, w, p: (0, (p[1] - d + 4) % 4, 0, (p[0] + w) % 2, 0, 0)
            ),
        ),
        input_output_aliases={12: 0},
        compiler_params=params(),
        cost_estimate=cost(8 * grad_a.size, 24 * grad_a.size),
        name="finish",
    )(pos, grad_a, grad_a, grad_b, *own, *other, into)


def per_device(
    hidden,
    cotangent,
    seq_ids,
    response_mask,
    group_ids,
    rewards,
    new_logp,
    old_logp,
    ref_logp,
    master,
):
    n_y, n_z = lax.axis_size("y"), lax.axis_size(("zh", "zl"))
    n_shard = lax.axis_size(SHARD)
    groups = lax.axis_size(REP) * n_shard * SEQ_DEV // 8
    layers, rows, kv = master.shape
    pos = jnp.stack([lax.axis_index(a).astype(jnp.int32) for a in ("c", "x", "zh", "y")])

    local_sums = group_sums(group_ids[0], rewards[0], groups)
    stats = sent_to_all(local_sums, REP).sum(axis=0)
    stats = sent_to_all(stats, SHARD)

    hidden_b = swapped(hidden)
    cotangent_b = swapped(cotangent)
    tok = token_rows(
        seq_ids[0], response_mask[0], group_ids[0], rewards[0], new_logp[0], old_logp[0], ref_logp[0]
    )
    tok_b = swapped(tok)

    partial = partial_product(pos, stats, tok.T, tok_b.T, cotangent, cotangent_b, hidden, hidden_b)
    to_x = spread_out(partial[:4], "x")
    to_y = spread_out(partial[4:], "y")
    to_y, to_x = sum_mid(pos, to_x, to_y)
    to_y = spread_out(to_y, "y")
    to_x = spread_out(to_x, "x")
    part = sum_turn(to_y, to_x)

    parts = rest_blocks(pos, master)
    parts = spread_out(parts, "zh")
    same, cross = regroup(pos, parts)
    rest = spread_out([same, cross, same, cross], "x")
    part = part.reshape(n_z, part.shape[0] // n_z, part.shape[1])
    zl = lax.axis_size("zl")
    part = exchanged(part, ("zh", "zl"))
    grad = exchanged(sum_spread(part, zl * n_y * 2), REP)
    grad = grad.reshape(zl, n_y, 2, *grad.shape[1:])
    first = send_blocks(pos, grad)
    first = exchanged(first.reshape(n_shard, *first.shape[3:]), SHARD)

    other = [swapped(r) for r in rest]
    out = place_rest(pos, rest, other, layers)
    entries = hidden.shape[1] * kv
    first_b = swapped(first)
    new_master = update(first, grad, master, entries)
    out = finish(pos, first, first_b, rest, other, out, entries)
    return (new_master, out.reshape(layers, n_shard * rows, 2 * HEAD))


def solution(mesh):
    split = Mesh(mesh.devices.reshape(2, 4, 2, 4, 4), REP + SHARD)
    row = P(REP + SHARD, None)
    return jax.shard_map(
        per_device,
        mesh=split,
        in_specs=(row,) * 9 + (P(None, SHARD, None),),
        out_specs=(P(SHARD, None), P(None, None, SHARD)),
        check_vma=False,
    )
```

```python
import jax
import jax.numpy as jnp
from jax import lax
from jax.experimental import pallas as pl
from jax.experimental.pallas import tpu as pltpu
from jax.sharding import Mesh
from jax.sharding import PartitionSpec as P

HEAD = 128
KV_HEADS = 4
SEQ_DEV = 4
LANES = 128
REP = ("zl", "y", "c")
SHARD = ("x", "zh")
VMEM_LIMIT = 24 * 1024 * 1024
f32 = jnp.float32
bf16 = jnp.bfloat16


def swapped(value):
    return lax.ppermute(value, "c", [(0, 1), (1, 0)])


def shifted(value, axis, by):
    n = lax.axis_size(axis)
    return lax.ppermute(value, axis, [(i, (i + by) % n) for i in range(n)])


def spread_out(blocks, axis):
    return [blocks[0]] + [shifted(blocks[d], axis, d) for d in range(1, 4)]


def exchanged(blocks, axis):
    return lax.all_to_all(blocks, axis, split_axis=0, concat_axis=0, tiled=True)


def sent_to_all(shard, axis):
    copies = jnp.broadcast_to(shard, (lax.axis_size(axis), *shard.shape))
    return exchanged(copies, axis)


def params(**kw):
    return pltpu.CompilerParams(vmem_limit_bytes=VMEM_LIMIT, **kw)


def cost(flops, nbytes):
    return pl.CostEstimate(flops=flops, bytes_accessed=nbytes, transcendentals=0)


def group_sums(group_flat, reward_flat, groups):
    onehot = (group_flat[:, None] == jnp.arange(groups, dtype=jnp.int32)[None, :]).astype(f32)
    values = jnp.stack([jnp.ones_like(reward_flat), reward_flat, reward_flat * reward_flat], axis=0)
    return jnp.dot(values, onehot, precision=lax.Precision.HIGHEST)


def token_rows(seq_row, mask_row, group_row, reward_row, new_row, old_row, ref_row):
    onehot = (seq_row[:, None] == jnp.arange(SEQ_DEV, dtype=jnp.int32)[None, :]).astype(f32)
    maskf = mask_row.astype(f32)
    lengths = jnp.maximum(jnp.dot(maskf, onehot, precision=lax.Precision.HIGHEST), 1.0)
    tok_len = jnp.dot(onehot, lengths, precision=lax.Precision.HIGHEST)
    tok_reward = jnp.dot(onehot, reward_row, precision=lax.Precision.HIGHEST)
    tok_group = jnp.dot(onehot, group_row.astype(f32), precision=lax.Precision.HIGHEST)
    weight = maskf / tok_len
    ratio = jnp.exp(new_row - old_row)
    penalty = 0.2 * (1.0 - jnp.exp(ref_row - new_row))
    zero = jnp.zeros_like(weight)
    return jnp.stack([weight, ratio, penalty, tok_reward, tok_group, zero, zero, zero], axis=0)


def turn_kernel(pos, cot_a, cot_b, out_a, out_b):
    half, _ = out_a.shape
    rows = half // 8
    cols = pl.ds(pl.multiple_of(pos[0] * half, half), half)
    for cot, out in ((cot_a, out_a), (cot_b, out_b)):
        turned = cot[:, cols].astype(f32).T.astype(bf16)
        for y in range(4):
            out[y * rows : (y + 1) * rows, :] = turned[2 * y * rows : (2 * y + 1) * rows]
            to = pl.multiple_of((4 + (y - pos[3] + 4) % 4) * rows, rows)
            out[pl.ds(to, rows), :] = turned[(2 * y + 1) * rows : (2 * y + 2) * rows]


def turn(pos, cot_a, cot_b):
    toks, kv = cot_a.shape
    whole = lambda *shape: pl.BlockSpec(shape, lambda i, p: (0,) * len(shape))
    return pl.pallas_call(
        turn_kernel,
        out_shape=[jax.ShapeDtypeStruct((kv // 2, toks), bf16)] * 2,
        grid_spec=pltpu.PrefetchScalarGridSpec(
            num_scalar_prefetch=1,
            grid=(1,),
            in_specs=[whole(toks, kv)] * 2,
            out_specs=[whole(kv // 2, toks)] * 2,
        ),
        compiler_params=params(),
        cost_estimate=cost(4 * cot_a.size, 6 * cot_a.size),
        name="turn",
    )(pos, cot_a, cot_b)


def partial_kernel(pos, stats, tok_a, tok_b, cot_a, cot_b, hid_a, hid_b, *refs):
    outs, (hid, sems) = refs[:8], refs[8:]
    rows, blk = outs[0].shape[1:]
    copies = []
    for d in range(4):
        cols = pl.ds(pl.multiple_of((pos[1] + d) % 4 * blk, LANES), blk)
        for k, src in enumerate((hid_a, hid_b)):
            copies.append(pltpu.make_async_copy(src.at[:, cols], hid.at[d, k], sems.at[d, k]))
    for copy in copies:
        copy.start()
    sums = jnp.sum(stats[...], axis=0)
    count = jnp.maximum(sums[0:1, :], 1.0)
    mean = sums[1:2, :] / count
    spread = jnp.maximum(jnp.sqrt(jnp.maximum(sums[2:3, :] / count - mean * mean, 0.0)), 0.5)
    table = jnp.concatenate([jnp.broadcast_to(mean, (8, LANES)), jnp.broadcast_to(spread, (8, LANES))], axis=0).T
    mean, spread = table[:, 0:1], table[:, 8:9]
    delta = []
    for tok, cot in ((tok_a, cot_a), (tok_b, cot_b)):
        t = tok[...]
        group = lax.broadcasted_iota(jnp.int32, (LANES, t.shape[1]), 0).astype(f32)
        pick = group == t[4:5]
        tok_mean = jnp.sum(jnp.where(pick, mean, 0.0), axis=0, keepdims=True)
        tok_std = jnp.sum(jnp.where(pick, spread, 0.0), axis=0, keepdims=True)
        adv = (t[3:4] - tok_mean) / tok_std
        coef = t[0:1] * (-adv * t[1:2] + t[2:3])
        delta.append((cot[...].astype(f32) * coef).astype(bf16))
    for d in range(4):
        copies[2 * d].wait()
        acc = jnp.dot(delta[0], hid[d, 0], preferred_element_type=f32)
        copies[2 * d + 1].wait()
        acc = acc + jnp.dot(delta[1], hid[d, 1], preferred_element_type=f32)
        acc = acc.astype(bf16).reshape(8, rows, blk)
        outs[d][...] = acc[:4]
        for e in range(4):
            outs[4 + e][(pos[1] + d) % 4] = acc[4 + e]


def partial_product(pos, stats, tok_a, tok_b, cot_a, cot_b, hid_a, hid_b):
    toks, width = hid_a.shape
    half = cot_a.shape[0]
    blk = width // 4
    shape = (4, half // 8, blk)
    whole = lambda s: pl.BlockSpec(s, lambda i, p: (0,) * len(s))
    far = pl.BlockSpec(memory_space=pltpu.HBM)
    return pl.pallas_call(
        partial_kernel,
        out_shape=[jax.ShapeDtypeStruct(shape, bf16)] * 8,
        grid_spec=pltpu.PrefetchScalarGridSpec(
            num_scalar_prefetch=1,
            grid=(1,),
            in_specs=[whole(a.shape) for a in (stats, tok_a, tok_b, cot_a, cot_b)] + [far, far],
            out_specs=[whole(shape)] * 8,
            scratch_shapes=[pltpu.VMEM((4, 2, toks, blk), bf16), pltpu.SemaphoreType.DMA((4, 2))],
        ),
        compiler_params=params(),
        cost_estimate=cost(4 * toks * width * half, 4 * toks * width + 2 * width * half),
        name="partial_product",
    )(pos, stats, tok_a, tok_b, cot_a, cot_b, hid_a, hid_b)


def sum_mid_kernel(axis, pos, *refs):
    srcs, outs = refs[:4], refs[4:]
    for d in range(4):
        k = (pos[axis] + d) % 4
        outs[d][...] = sum(src[k].astype(f32) for src in srcs).astype(bf16)


def sum_mid(pos, parts, axis):
    _, rows, width = parts[0].shape
    whole = lambda *shape: pl.BlockSpec(shape, lambda i, p: (0,) * len(shape))
    return pl.pallas_call(
        lambda *refs: sum_mid_kernel(axis, *refs),
        out_shape=[jax.ShapeDtypeStruct((rows, width), bf16)] * 4,
        grid_spec=pltpu.PrefetchScalarGridSpec(
            num_scalar_prefetch=1,
            grid=(1,),
            in_specs=[whole(4, rows, width)] * 4,
            out_specs=[whole(rows, width)] * 4,
        ),
        compiler_params=params(),
        cost_estimate=cost(16 * rows * width, 40 * rows * width),
    )(pos, *parts)


def sum_turn_kernel(*refs):
    srcs, out = refs[:8], refs[8]
    first = sum(src[...].astype(f32) for src in srcs[:4])
    second = sum(src[...].astype(f32) for src in srcs[4:])
    out[...] = jnp.concatenate([first, second], axis=0).T.astype(bf16)


def sum_turn(first, second):
    rows, width = first[0].shape
    return pl.pallas_call(
        sum_turn_kernel,
        out_shape=jax.ShapeDtypeStruct((width, 2 * rows), bf16),
        compiler_params=params(),
        cost_estimate=cost(8 * rows * width, 20 * rows * width),
        name="sum_turn",
    )(*first, *second)


def sum_spread_kernel(src, out):
    total = jnp.sum(src[...].astype(f32), axis=0).astype(bf16)
    for i in range(out.shape[0]):
        out[i] = total


def sum_spread(blocks, copies):
    n, rows, width = blocks.shape
    return pl.pallas_call(
        sum_spread_kernel,
        out_shape=jax.ShapeDtypeStruct((copies, rows, width), bf16),
        compiler_params=params(),
        cost_estimate=cost(n * rows * width, 4 * n * rows * width),
        name="sum_spread",
    )(blocks)


def send_kernel(pos, grad, blocks):
    g = grad[...].astype(f32)
    s = jnp.sum(g * g, axis=(0, 1, 2))
    s = jnp.sum(jnp.sum(s, axis=0, keepdims=True), axis=1, keepdims=True)
    high = s.astype(bf16).astype(f32)
    mid = (s - high).astype(bf16).astype(f32)
    low = s - high - mid
    rows = grad.shape[3]
    row = lax.broadcasted_iota(jnp.int32, (8, 2 * HEAD), 0)
    tail = jnp.where(row == 0, high, jnp.where(row == 1, mid, jnp.where(row == 2, low, 0.0))).astype(bf16)
    for h in range(KV_HEADS):
        for i in range(2):
            for j in range(2):
                for kv in range(2):
                    blocks[i, h, j, :rows, kv * HEAD : (kv + 1) * HEAD] = grad[pos[0], h, kv]
                blocks[i, h, j, rows:, :] = tail


def send_blocks(pos, grad):
    rows = grad.shape[3]
    whole = lambda s: pl.BlockSpec(s, lambda i, p: (0,) * len(s))
    shape = (2, KV_HEADS, 2, rows + 8, 2 * HEAD)
    return pl.pallas_call(
        send_kernel,
        out_shape=jax.ShapeDtypeStruct(shape, bf16),
        grid_spec=pltpu.PrefetchScalarGridSpec(
            num_scalar_prefetch=1, grid=(1,), in_specs=[whole(grad.shape)], out_specs=whole(shape)
        ),
        compiler_params=params(),
        cost_estimate=cost(4 * grad.size, 8 * grad.size),
        name="send_blocks",
    )(pos, grad)


def step_size(squares, entries):
    s = jnp.sum(squares[...].astype(f32), axis=0)[:, 0:1]
    total = s[0:1] + s[1:2] + s[2:3]
    return 0.5 / jnp.sqrt(total / entries + 1e-06)


def update_kernel(entries, squares, grad, master, new):
    zl, ny, _, rows, width = grad.shape
    step = step_size(squares, entries)
    for kv in range(2):
        for y in range(ny):
            for z in range(zl):
                r = slice(z * rows, (z + 1) * rows)
                c = slice((kv * ny + y) * width, (kv * ny + y + 1) * width)
                new[r, c] = master[0, r, c] - grad[z, y, kv].astype(f32) * step


def update(received, grad, master, entries):
    _, rows, kv = master.shape
    return pl.pallas_call(
        lambda *refs: update_kernel(entries, *refs),
        out_shape=jax.ShapeDtypeStruct((rows, kv), f32),
        grid=(1,),
        in_specs=[
            pl.BlockSpec((received.shape[0], 8, LANES), lambda i: (0, rows // 16, 0)),
            pl.BlockSpec(grad.shape, lambda i: (0, 0, 0, 0, 0)),
            pl.BlockSpec((1, rows, kv), lambda i: (0, 0, 0)),
        ],
        out_specs=pl.BlockSpec((rows, kv), lambda i: (0, 0)),
        compiler_params=params(),
        cost_estimate=cost(4 * rows * kv, 10 * rows * kv),
        name="update",
    )(received, grad, master)


def rest_kernel(pos, *refs):
    masters, outs = refs[:8], refs[8:]
    for d in range(4):
        for kv in range(2):
            outs[d][0, :, :, kv * HEAD : (kv + 1) * HEAD] = masters[2 * d + kv][...].astype(bf16)


def rest_blocks(pos, master):
    layers, rows, kv = master.shape
    half = rows // 2

    def spec(d, k):
        return pl.BlockSpec(
            (layers, half, HEAD),
            lambda xl, p: (0, p[0], k * KV_HEADS + xl * 2 + ((p[2] + d) % 4) // 2),
        )

    shape = (2, layers, half, 2 * HEAD)
    return pl.pallas_call(
        rest_kernel,
        out_shape=[jax.ShapeDtypeStruct(shape, bf16)] * 4,
        grid_spec=pltpu.PrefetchScalarGridSpec(
            num_scalar_prefetch=1,
            grid=(2,),
            in_specs=[spec(d, k) for d in range(4) for k in range(2)],
            out_specs=[pl.BlockSpec((1, *shape[1:]), lambda xl, p: (xl, 0, 0, 0))] * 4,
        ),
        compiler_params=params(),
        cost_estimate=cost(layers * rows * kv, 12 * rows * kv),
        name="rest_blocks",
    )(pos, *([master] * 8))


def regroup_kernel(pos, *refs):
    parts, (same, cross), sems = refs[:4], refs[4:6], refs[6]
    xl = pos[1] % 2
    copies = []
    for d in range(4):
        copies.append(pltpu.make_async_copy(parts[d].at[xl], same.at[d], sems.at[2 * d]))
        copies.append(pltpu.make_async_copy(parts[d].at[1 - xl], cross.at[d], sems.at[2 * d + 1]))
    for copy in copies:
        copy.start()
    for copy in copies:
        copy.wait()


def regroup(pos, parts):
    shape = (4, *parts[0].shape[1:])
    whole = lambda s: pl.BlockSpec(s, lambda i, p: (0,) * len(s))
    return pl.pallas_call(
        regroup_kernel,
        out_shape=[jax.ShapeDtypeStruct(shape, bf16)] * 2,
        grid_spec=pltpu.PrefetchScalarGridSpec(
            num_scalar_prefetch=1,
            grid=(1,),
            in_specs=[pl.BlockSpec(memory_space=pltpu.HBM)] * 4,
            out_specs=[whole(shape)] * 2,
            scratch_shapes=[pltpu.SemaphoreType.DMA((8,))],
        ),
        compiler_params=params(),
        cost_estimate=cost(parts[0].size, 16 * parts[0].size),
        name="regroup",
    )(pos, *parts)


def place_rest_kernel(pos, *refs):
    srcs, out = refs[:8], refs[8]
    zh, core = pos[2], pos[0]
    for dx in range(4):

        @pl.when(pl.program_id(1) == dx)
        def _():
            for w in range(2):
                for dz in range(4):
                    out[0, 0, (zh - dz + 4) % 4, (core + w) % 2] = srcs[4 * w + dx][dz, 0]


def place_rest(pos, own, other, layers):
    _, count, half, width = own[0].shape
    src = pl.BlockSpec((4, 1, half, width), lambda l, d, p: (0, 1 + l, 0, 0))
    return pl.pallas_call(
        place_rest_kernel,
        out_shape=jax.ShapeDtypeStruct((layers, 4, 4, 2, half, width), bf16),
        grid_spec=pltpu.PrefetchScalarGridSpec(
            num_scalar_prefetch=1,
            grid=(count - 1, 4),
            in_specs=[src] * 8,
            out_specs=pl.BlockSpec(
                (1, 1, 4, 2, half, width), lambda l, d, p: (1 + l, (p[1] - d + 4) % 4, 0, 0, 0, 0)
            ),
        ),
        compiler_params=params(),
        cost_estimate=cost(own[0].size, 32 * own[0].size),
        name="place_rest",
    )(pos, *own, *other)


def finish_kernel(entries, pos, squares, grad_a, grad_b, *refs):
    masters, out = refs[:8], refs[9]
    zh, core = pos[2], pos[0]
    step = step_size(squares, entries)
    half = out.shape[4]
    for dx in range(4):

        @pl.when(pl.program_id(0) == dx)
        def _():
            for w in range(2):
                grad = (grad_a, grad_b)[w]
                for dz in range(4):
                    k = (zh - dz + 4) % 4
                    value = masters[4 * w + dx][dz, 0].astype(f32) - grad[k, :half].astype(f32) * step
                    out[0, 0, k, (core + w) % 2] = value.astype(bf16)


def finish(pos, grad_a, grad_b, own, other, into, entries):
    n, padded, width = grad_a.shape
    half = padded - 8
    grad = pl.BlockSpec((4, padded, width), lambda d, p: ((p[1] - d + 4) % 4, 0, 0))
    src = pl.BlockSpec((4, 1, half, width), lambda d, p: (0, 0, 0, 0))
    return pl.pallas_call(
        lambda *refs: finish_kernel(entries, *refs),
        out_shape=jax.ShapeDtypeStruct(into.shape, bf16),
        grid_spec=pltpu.PrefetchScalarGridSpec(
            num_scalar_prefetch=1,
            grid=(4,),
            in_specs=[pl.BlockSpec((n, 8, LANES), lambda d, p: (0, half // 8, 0)), grad, grad]
            + [src] * 8
            + [pl.BlockSpec(memory_space=pl.ANY)],
            out_specs=pl.BlockSpec(
                (1, 1, 4, 2, half, width), lambda d, p: (0, (p[1] - d + 4) % 4, 0, 0, 0, 0)
            ),
        ),
        input_output_aliases={12: 0},
        compiler_params=params(),
        cost_estimate=cost(8 * grad_a.size, 24 * grad_a.size),
        name="finish",
    )(pos, grad_a, grad_a, grad_b, *own, *other, into)


def per_device(
    hidden,
    cotangent,
    seq_ids,
    response_mask,
    group_ids,
    rewards,
    new_logp,
    old_logp,
    ref_logp,
    master,
):
    n_y, n_z = lax.axis_size("y"), lax.axis_size(("zh", "zl"))
    n_shard = lax.axis_size(SHARD)
    groups = lax.axis_size(REP) * n_shard * SEQ_DEV // 8
    layers, rows, kv = master.shape
    pos = jnp.stack([lax.axis_index(a).astype(jnp.int32) for a in ("c", "x", "zh", "y")])

    local_sums = group_sums(group_ids[0], rewards[0], groups)
    stats = sent_to_all(local_sums, REP).sum(axis=0)
    stats = sent_to_all(stats, SHARD)

    hidden_b = swapped(hidden)
    cotangent_b = swapped(cotangent)
    tok = token_rows(
        seq_ids[0], response_mask[0], group_ids[0], rewards[0], new_logp[0], old_logp[0], ref_logp[0]
    )
    tok_b = swapped(tok)

    turned = turn(pos, cotangent, cotangent_b)
    partial = partial_product(pos, stats, tok, tok_b, *turned, hidden, hidden_b)
    to_x = spread_out(partial[:4], "x")
    to_y = spread_out(partial[4:], "y")
    to_x = sum_mid(pos, to_x, 3)
    to_x = spread_out(to_x, "y")
    to_y = sum_mid(pos, to_y, 1)
    to_y = spread_out(to_y, "x")
    part = sum_turn(to_x, to_y)

    parts = rest_blocks(pos, master)
    parts = spread_out(parts, "zh")
    same, cross = regroup(pos, parts)
    rest = spread_out([same, cross, same, cross], "x")
    part = part.reshape(n_z, part.shape[0] // n_z, part.shape[1])
    zl = lax.axis_size("zl")
    part = exchanged(part, ("zh", "zl"))
    grad = exchanged(sum_spread(part, zl * n_y * 2), REP)
    grad = grad.reshape(zl, n_y, 2, *grad.shape[1:])
    first = send_blocks(pos, grad)
    first = exchanged(first.reshape(n_shard, *first.shape[3:]), SHARD)

    other = [swapped(r) for r in rest]
    out = place_rest(pos, rest, other, layers)
    entries = hidden.shape[1] * kv
    first_b = swapped(first)
    new_master = update(first, grad, master, entries)
    out = finish(pos, first, first_b, rest, other, out, entries)
    return (new_master, out.reshape(layers, n_shard * rows, 2 * HEAD))


def solution(mesh):
    split = Mesh(mesh.devices.reshape(2, 4, 2, 4, 4), REP + SHARD)
    row = P(REP + SHARD, None)
    return jax.shard_map(
        per_device,
        mesh=split,
        in_specs=(row,) * 9 + (P(None, SHARD, None),),
        out_specs=(P(SHARD, None), P(None, None, SHARD)),
        check_vma=False,
    )
```

```python
import jax
import jax.numpy as jnp
from jax import lax
from jax.experimental import pallas as pl
from jax.experimental.pallas import tpu as pltpu
from jax.sharding import Mesh
from jax.sharding import PartitionSpec as P

HEAD = 128
KV_HEADS = 4
SEQ_DEV = 4
LANES = 128
REP = ("zl", "y", "c")
SHARD = ("x", "zh")
VMEM_LIMIT = 24 * 1024 * 1024
f32 = jnp.float32
bf16 = jnp.bfloat16


def swapped(value):
    return lax.ppermute(value, "c", [(0, 1), (1, 0)])


def shifted(value, axis, by):
    n = lax.axis_size(axis)
    return lax.ppermute(value, axis, [(i, (i + by) % n) for i in range(n)])


def spread_out(blocks, axis):
    return [blocks[0]] + [shifted(blocks[d], axis, d) for d in range(1, 4)]


def exchanged(blocks, axis):
    return lax.all_to_all(blocks, axis, split_axis=0, concat_axis=0, tiled=True)


def sent_to_all(shard, axis):
    copies = jnp.broadcast_to(shard, (lax.axis_size(axis), *shard.shape))
    return exchanged(copies, axis)


def params(limit=VMEM_LIMIT):
    return pltpu.CompilerParams(vmem_limit_bytes=limit)


def cost(flops, nbytes):
    return pl.CostEstimate(flops=flops, bytes_accessed=nbytes, transcendentals=0)


def group_sums(group_flat, reward_flat, groups):
    onehot = (group_flat[:, None] == jnp.arange(groups, dtype=jnp.int32)[None, :]).astype(f32)
    values = jnp.stack([jnp.ones_like(reward_flat), reward_flat, reward_flat * reward_flat], axis=0)
    return jnp.dot(values, onehot, precision=lax.Precision.HIGHEST)


def token_rows(seq_row, mask_row, group_row, reward_row, new_row, old_row, ref_row):
    onehot = (seq_row[:, None] == jnp.arange(SEQ_DEV, dtype=jnp.int32)[None, :]).astype(f32)
    maskf = mask_row.astype(f32)
    lengths = jnp.maximum(jnp.dot(maskf, onehot, precision=lax.Precision.HIGHEST), 1.0)
    tok_len = jnp.dot(onehot, lengths, precision=lax.Precision.HIGHEST)
    tok_reward = jnp.dot(onehot, reward_row, precision=lax.Precision.HIGHEST)
    tok_group = jnp.dot(onehot, group_row.astype(f32), precision=lax.Precision.HIGHEST)
    weight = maskf / tok_len
    ratio = jnp.exp(new_row - old_row)
    penalty = 0.2 * (1.0 - jnp.exp(ref_row - new_row))
    zero = jnp.zeros_like(weight)
    return jnp.stack([weight, ratio, penalty, tok_reward, tok_group, zero, zero, zero], axis=0)


def turn_kernel(pos, cot_a, cot_b, out_a, out_b):
    half, _ = out_a.shape
    rows = half // 8
    cols = pl.ds(pl.multiple_of(pos[0] * half, half), half)
    for cot, out in ((cot_a, out_a), (cot_b, out_b)):
        turned = cot[:, cols].astype(f32).T.astype(bf16)
        for y in range(4):
            out[y * rows : (y + 1) * rows, :] = turned[2 * y * rows : (2 * y + 1) * rows]
            to = pl.multiple_of((4 + (y - pos[3] + 4) % 4) * rows, rows)
            out[pl.ds(to, rows), :] = turned[(2 * y + 1) * rows : (2 * y + 2) * rows]


def turn(pos, cot_a, cot_b):
    toks, kv = cot_a.shape
    whole = lambda *shape: pl.BlockSpec(shape, lambda i, p: (0,) * len(shape))
    return pl.pallas_call(
        turn_kernel,
        out_shape=[jax.ShapeDtypeStruct((kv // 2, toks), bf16)] * 2,
        grid_spec=pltpu.PrefetchScalarGridSpec(
            num_scalar_prefetch=1,
            grid=(1,),
            in_specs=[whole(toks, kv)] * 2,
            out_specs=[whole(kv // 2, toks)] * 2,
        ),
        compiler_params=params(),
        cost_estimate=cost(4 * cot_a.size, 6 * cot_a.size),
        name="turn",
    )(pos, cot_a, cot_b)


def partial_kernel(pos, stats, tok_a, tok_b, cot_a, cot_b, hid_a, hid_b, *refs):
    outs, (hid, sems) = refs[:8], refs[8:]
    rows, blk = outs[0].shape[1:]
    copies = []
    for d in range(4):
        cols = pl.ds(pl.multiple_of((pos[1] + d) % 4 * blk, LANES), blk)
        for k, src in enumerate((hid_a, hid_b)):
            copies.append(pltpu.make_async_copy(src.at[:, cols], hid.at[d, k], sems.at[d, k]))
    for copy in copies:
        copy.start()
    sums = jnp.sum(stats[...], axis=0)
    count = jnp.maximum(sums[0:1, :], 1.0)
    mean = sums[1:2, :] / count
    spread = jnp.maximum(jnp.sqrt(jnp.maximum(sums[2:3, :] / count - mean * mean, 0.0)), 0.5)
    table = jnp.concatenate([jnp.broadcast_to(mean, (8, LANES)), jnp.broadcast_to(spread, (8, LANES))], axis=0).T
    mean, spread = table[:, 0:1], table[:, 8:9]
    delta = []
    for tok, cot in ((tok_a, cot_a), (tok_b, cot_b)):
        t = tok[...]
        group = lax.broadcasted_iota(jnp.int32, (LANES, t.shape[1]), 0).astype(f32)
        pick = group == t[4:5]
        tok_mean = jnp.sum(jnp.where(pick, mean, 0.0), axis=0, keepdims=True)
        tok_std = jnp.sum(jnp.where(pick, spread, 0.0), axis=0, keepdims=True)
        adv = (t[3:4] - tok_mean) / tok_std
        coef = t[0:1] * (-adv * t[1:2] + t[2:3])
        delta.append((cot[...].astype(f32) * coef).astype(bf16))
    for d in range(4):
        copies[2 * d].wait()
        acc = jnp.dot(delta[0], hid[d, 0], preferred_element_type=f32)
        copies[2 * d + 1].wait()
        acc = acc + jnp.dot(delta[1], hid[d, 1], preferred_element_type=f32)
        acc = acc.astype(bf16).reshape(8, rows, blk)
        outs[d][...] = acc[:4]
        for e in range(4):
            outs[4 + e][(pos[1] + d) % 4] = acc[4 + e]


def partial_product(pos, stats, tok_a, tok_b, cot_a, cot_b, hid_a, hid_b):
    toks, width = hid_a.shape
    half = cot_a.shape[0]
    blk = width // 4
    shape = (4, half // 8, blk)
    whole = lambda s: pl.BlockSpec(s, lambda i, p: (0,) * len(s))
    far = pl.BlockSpec(memory_space=pltpu.HBM)
    return pl.pallas_call(
        partial_kernel,
        out_shape=[jax.ShapeDtypeStruct(shape, bf16)] * 8,
        grid_spec=pltpu.PrefetchScalarGridSpec(
            num_scalar_prefetch=1,
            grid=(1,),
            in_specs=[whole(a.shape) for a in (stats, tok_a, tok_b, cot_a, cot_b)] + [far, far],
            out_specs=[whole(shape)] * 8,
            scratch_shapes=[pltpu.VMEM((4, 2, toks, blk), bf16), pltpu.SemaphoreType.DMA((4, 2))],
        ),
        compiler_params=params(50 * 1024 * 1024),
        cost_estimate=cost(4 * toks * width * half, 4 * toks * width + 2 * width * half),
        name="partial_product",
    )(pos, stats, tok_a, tok_b, cot_a, cot_b, hid_a, hid_b)


def sum_mid_kernel(axis, pos, *refs):
    srcs, outs = refs[:4], refs[4:]
    for d in range(4):
        k = (pos[axis] + d) % 4
        outs[d][...] = sum(src[k].astype(f32) for src in srcs).astype(bf16)


def sum_mid(pos, parts, axis):
    _, rows, width = parts[0].shape
    whole = lambda *shape: pl.BlockSpec(shape, lambda i, p: (0,) * len(shape))
    return pl.pallas_call(
        lambda *refs: sum_mid_kernel(axis, *refs),
        out_shape=[jax.ShapeDtypeStruct((rows, width), bf16)] * 4,
        grid_spec=pltpu.PrefetchScalarGridSpec(
            num_scalar_prefetch=1,
            grid=(1,),
            in_specs=[whole(4, rows, width)] * 4,
            out_specs=[whole(rows, width)] * 4,
        ),
        compiler_params=params(),
        cost_estimate=cost(16 * rows * width, 40 * rows * width),
    )(pos, *parts)


def sum_turn_kernel(*refs):
    srcs, out = refs[:8], refs[8]
    first = sum(src[...].astype(f32) for src in srcs[:4])
    second = sum(src[...].astype(f32) for src in srcs[4:])
    out[...] = jnp.concatenate([first, second], axis=0).T.astype(bf16)


def sum_turn(first, second):
    rows, width = first[0].shape
    return pl.pallas_call(
        sum_turn_kernel,
        out_shape=jax.ShapeDtypeStruct((width, 2 * rows), bf16),
        compiler_params=params(),
        cost_estimate=cost(8 * rows * width, 20 * rows * width),
        name="sum_turn",
    )(*first, *second)


def sum_spread_kernel(src, out):
    total = jnp.sum(src[...].astype(f32), axis=0).astype(bf16)
    for i in range(out.shape[0]):
        out[i] = total


def sum_spread(blocks, copies):
    n, rows, width = blocks.shape
    return pl.pallas_call(
        sum_spread_kernel,
        out_shape=jax.ShapeDtypeStruct((copies, rows, width), bf16),
        compiler_params=params(),
        cost_estimate=cost(n * rows * width, 4 * n * rows * width),
        name="sum_spread",
    )(blocks)


def send_kernel(pos, grad, blocks):
    g = grad[...].astype(f32)
    s = jnp.sum(g * g, axis=(0, 1, 2))
    s = jnp.sum(jnp.sum(s, axis=0, keepdims=True), axis=1, keepdims=True)
    high = s.astype(bf16).astype(f32)
    mid = (s - high).astype(bf16).astype(f32)
    low = s - high - mid
    rows = grad.shape[3]
    row = lax.broadcasted_iota(jnp.int32, (8, 2 * HEAD), 0)
    tail = jnp.where(row == 0, high, jnp.where(row == 1, mid, jnp.where(row == 2, low, 0.0))).astype(bf16)
    for h in range(KV_HEADS):
        for i in range(2):
            for j in range(2):
                for kv in range(2):
                    blocks[i, h, j, :rows, kv * HEAD : (kv + 1) * HEAD] = grad[pos[0], h, kv]
                blocks[i, h, j, rows:, :] = tail


def send_blocks(pos, grad):
    rows = grad.shape[3]
    whole = lambda s: pl.BlockSpec(s, lambda i, p: (0,) * len(s))
    shape = (2, KV_HEADS, 2, rows + 8, 2 * HEAD)
    return pl.pallas_call(
        send_kernel,
        out_shape=jax.ShapeDtypeStruct(shape, bf16),
        grid_spec=pltpu.PrefetchScalarGridSpec(
            num_scalar_prefetch=1, grid=(1,), in_specs=[whole(grad.shape)], out_specs=whole(shape)
        ),
        compiler_params=params(),
        cost_estimate=cost(4 * grad.size, 8 * grad.size),
        name="send_blocks",
    )(pos, grad)


def step_size(squares, entries):
    s = jnp.sum(squares[...].astype(f32), axis=0)[:, 0:1]
    total = s[0:1] + s[1:2] + s[2:3]
    return 0.5 / jnp.sqrt(total / entries + 1e-06)


def update_kernel(entries, squares, grad, master, new):
    zl, ny, _, rows, width = grad.shape
    step = step_size(squares, entries)
    for kv in range(2):
        for y in range(ny):
            for z in range(zl):
                r = slice(z * rows, (z + 1) * rows)
                c = slice((kv * ny + y) * width, (kv * ny + y + 1) * width)
                new[r, c] = master[0, r, c] - grad[z, y, kv].astype(f32) * step


def update(received, grad, master, entries):
    _, rows, kv = master.shape
    return pl.pallas_call(
        lambda *refs: update_kernel(entries, *refs),
        out_shape=jax.ShapeDtypeStruct((rows, kv), f32),
        grid=(1,),
        in_specs=[
            pl.BlockSpec((received.shape[0], 8, LANES), lambda i: (0, rows // 16, 0)),
            pl.BlockSpec(grad.shape, lambda i: (0, 0, 0, 0, 0)),
            pl.BlockSpec((1, rows, kv), lambda i: (0, 0, 0)),
        ],
        out_specs=pl.BlockSpec((rows, kv), lambda i: (0, 0)),
        compiler_params=params(),
        cost_estimate=cost(4 * rows * kv, 10 * rows * kv),
        name="update",
    )(received, grad, master)


def rest_kernel(pos, *refs):
    masters, outs = refs[:8], refs[8:]
    for d in range(4):
        for kv in range(2):
            outs[d][0, :, :, kv * HEAD : (kv + 1) * HEAD] = masters[2 * d + kv][...].astype(bf16)


def rest_blocks(pos, master):
    layers, rows, kv = master.shape
    half = rows // 2

    def spec(d, k):
        return pl.BlockSpec(
            (layers, half, HEAD),
            lambda xl, p: (0, p[0], k * KV_HEADS + xl * 2 + ((p[2] + d) % 4) // 2),
        )

    shape = (2, layers, half, 2 * HEAD)
    return pl.pallas_call(
        rest_kernel,
        out_shape=[jax.ShapeDtypeStruct(shape, bf16)] * 4,
        grid_spec=pltpu.PrefetchScalarGridSpec(
            num_scalar_prefetch=1,
            grid=(2,),
            in_specs=[spec(d, k) for d in range(4) for k in range(2)],
            out_specs=[pl.BlockSpec((1, *shape[1:]), lambda xl, p: (xl, 0, 0, 0))] * 4,
        ),
        compiler_params=params(),
        cost_estimate=cost(layers * rows * kv, 12 * rows * kv),
        name="rest_blocks",
    )(pos, *([master] * 8))


def regroup_kernel(pos, *refs):
    parts, (same, cross), sems = refs[:4], refs[4:6], refs[6]
    xl = pos[1] % 2
    copies = []
    for d in range(4):
        copies.append(pltpu.make_async_copy(parts[d].at[xl], same.at[d], sems.at[2 * d]))
        copies.append(pltpu.make_async_copy(parts[d].at[1 - xl], cross.at[d], sems.at[2 * d + 1]))
    for copy in copies:
        copy.start()
    for copy in copies:
        copy.wait()


def regroup(pos, parts):
    shape = (4, *parts[0].shape[1:])
    whole = lambda s: pl.BlockSpec(s, lambda i, p: (0,) * len(s))
    return pl.pallas_call(
        regroup_kernel,
        out_shape=[jax.ShapeDtypeStruct(shape, bf16)] * 2,
        grid_spec=pltpu.PrefetchScalarGridSpec(
            num_scalar_prefetch=1,
            grid=(1,),
            in_specs=[pl.BlockSpec(memory_space=pltpu.HBM)] * 4,
            out_specs=[whole(shape)] * 2,
            scratch_shapes=[pltpu.SemaphoreType.DMA((8,))],
        ),
        compiler_params=params(),
        cost_estimate=cost(parts[0].size, 16 * parts[0].size),
        name="regroup",
    )(pos, *parts)


def place_rest_kernel(pos, *refs):
    srcs, out = refs[:8], refs[8]
    zh, core = pos[2], pos[0]
    for dx in range(4):

        @pl.when(pl.program_id(1) == dx)
        def _():
            for w in range(2):
                for dz in range(4):
                    out[0, 0, (zh - dz + 4) % 4, (core + w) % 2] = srcs[4 * w + dx][dz, 0]


def place_rest(pos, own, other, layers):
    _, count, half, width = own[0].shape
    src = pl.BlockSpec((4, 1, half, width), lambda l, d, p: (0, 1 + l, 0, 0))
    return pl.pallas_call(
        place_rest_kernel,
        out_shape=jax.ShapeDtypeStruct((layers, 4, 4, 2, half, width), bf16),
        grid_spec=pltpu.PrefetchScalarGridSpec(
            num_scalar_prefetch=1,
            grid=(count - 1, 4),
            in_specs=[src] * 8,
            out_specs=pl.BlockSpec(
                (1, 1, 4, 2, half, width), lambda l, d, p: (1 + l, (p[1] - d + 4) % 4, 0, 0, 0, 0)
            ),
        ),
        compiler_params=params(),
        cost_estimate=cost(own[0].size, 32 * own[0].size),
        name="place_rest",
    )(pos, *own, *other)


def finish_kernel(entries, pos, squares, grad_a, grad_b, *refs):
    masters, out = refs[:8], refs[9]
    zh, core = pos[2], pos[0]
    step = step_size(squares, entries)
    half = out.shape[4]
    for dx in range(4):

        @pl.when(pl.program_id(0) == dx)
        def _():
            for w in range(2):
                grad = (grad_a, grad_b)[w]
                for dz in range(4):
                    k = (zh - dz + 4) % 4
                    value = masters[4 * w + dx][dz, 0].astype(f32) - grad[k, :half].astype(f32) * step
                    out[0, 0, k, (core + w) % 2] = value.astype(bf16)


def finish(pos, grad_a, grad_b, own, other, into, entries):
    n, padded, width = grad_a.shape
    half = padded - 8
    grad = pl.BlockSpec((4, padded, width), lambda d, p: ((p[1] - d + 4) % 4, 0, 0))
    src = pl.BlockSpec((4, 1, half, width), lambda d, p: (0, 0, 0, 0))
    return pl.pallas_call(
        lambda *refs: finish_kernel(entries, *refs),
        out_shape=jax.ShapeDtypeStruct(into.shape, bf16),
        grid_spec=pltpu.PrefetchScalarGridSpec(
            num_scalar_prefetch=1,
            grid=(4,),
            in_specs=[pl.BlockSpec((n, 8, LANES), lambda d, p: (0, half // 8, 0)), grad, grad]
            + [src] * 8
            + [pl.BlockSpec(memory_space=pl.ANY)],
            out_specs=pl.BlockSpec(
                (1, 1, 4, 2, half, width), lambda d, p: (0, (p[1] - d + 4) % 4, 0, 0, 0, 0)
            ),
        ),
        input_output_aliases={12: 0},
        compiler_params=params(),
        cost_estimate=cost(8 * grad_a.size, 24 * grad_a.size),
        name="finish",
    )(pos, grad_a, grad_a, grad_b, *own, *other, into)


def per_device(
    hidden,
    cotangent,
    seq_ids,
    response_mask,
    group_ids,
    rewards,
    new_logp,
    old_logp,
    ref_logp,
    master,
):
    n_y, n_z = lax.axis_size("y"), lax.axis_size(("zh", "zl"))
    n_shard = lax.axis_size(SHARD)
    groups = lax.axis_size(REP) * n_shard * SEQ_DEV // 8
    layers, rows, kv = master.shape
    pos = jnp.stack([lax.axis_index(a).astype(jnp.int32) for a in ("c", "x", "zh", "y")])

    local_sums = group_sums(group_ids[0], rewards[0], groups)
    stats = sent_to_all(local_sums, ("x", "y")).sum(axis=0)
    stats = sent_to_all(stats, ("zh", "zl", "c"))

    hidden_b = swapped(hidden)
    cotangent_b = swapped(cotangent)
    tok = token_rows(
        seq_ids[0], response_mask[0], group_ids[0], rewards[0], new_logp[0], old_logp[0], ref_logp[0]
    )
    tok_b = swapped(tok)

    turned = turn(pos, cotangent, cotangent_b)
    partial = partial_product(pos, stats, tok, tok_b, *turned, hidden, hidden_b)
    to_x = spread_out(partial[:4], "x")
    to_y = spread_out(partial[4:], "y")
    to_x = sum_mid(pos, to_x, 3)
    to_x = spread_out(to_x, "y")
    to_y = sum_mid(pos, to_y, 1)
    to_y = spread_out(to_y, "x")
    part = sum_turn(to_x, to_y)

    parts = rest_blocks(pos, master)
    parts = spread_out(parts, "zh")
    same, cross = regroup(pos, parts)
    rest = spread_out([same, cross, same, cross], "x")
    part = part.reshape(n_z, part.shape[0] // n_z, part.shape[1])
    zl = lax.axis_size("zl")
    part = exchanged(part, ("zh", "zl"))
    grad = exchanged(sum_spread(part, zl * n_y * 2), REP)
    grad = grad.reshape(zl, n_y, 2, *grad.shape[1:])
    first = send_blocks(pos, grad)
    first = exchanged(first.reshape(n_shard, *first.shape[3:]), SHARD)

    other = [swapped(r) for r in rest]
    out = place_rest(pos, rest, other, layers)
    entries = hidden.shape[1] * kv
    first_b = swapped(first)
    new_master = update(first, grad, master, entries)
    out = finish(pos, first, first_b, rest, other, out, entries)
    return (new_master, out.reshape(layers, n_shard * rows, 2 * HEAD))


def solution(mesh):
    split = Mesh(mesh.devices.reshape(2, 4, 2, 4, 4), REP + SHARD)
    row = P(REP + SHARD, None)
    return jax.shard_map(
        per_device,
        mesh=split,
        in_specs=(row,) * 9 + (P(None, SHARD, None),),
        out_specs=(P(SHARD, None), P(None, None, SHARD)),
        check_vma=False,
    )
```

```python
import jax
import jax.numpy as jnp
from jax import lax
from jax.experimental import pallas as pl
from jax.experimental.pallas import tpu as pltpu
from jax.sharding import Mesh
from jax.sharding import PartitionSpec as P

HEAD = 128
KV_HEADS = 4
SEQ_DEV = 4
LANES = 128
REP = ("zl", "y", "c")
SHARD = ("x", "zh")
VMEM_LIMIT = 24 * 1024 * 1024
f32 = jnp.float32
bf16 = jnp.bfloat16


def swapped(value):
    return lax.ppermute(value, "c", [(0, 1), (1, 0)])


def shifted(value, axis, by):
    n = lax.axis_size(axis)
    return lax.ppermute(value, axis, [(i, (i + by) % n) for i in range(n)])


def spread_out(blocks, axis):
    return [blocks[0]] + [shifted(blocks[d], axis, d) for d in range(1, 4)]


def exchanged(blocks, axis):
    return lax.all_to_all(blocks, axis, split_axis=0, concat_axis=0, tiled=True)


def params(limit=VMEM_LIMIT):
    return pltpu.CompilerParams(vmem_limit_bytes=limit)


def cost(flops, nbytes):
    return pl.CostEstimate(flops=flops, bytes_accessed=nbytes, transcendentals=0)


def sums_kernel(group, reward, out):
    lane = lax.broadcasted_iota(jnp.int32, (1, LANES), 1)
    count = total = squares = jnp.zeros((1, LANES), f32)
    for k in range(SEQ_DEV):
        value = reward[:, k : k + 1]
        mine = lane == group[:, k : k + 1]
        count = count + jnp.where(mine, 1.0, 0.0)
        total = total + jnp.where(mine, value, 0.0)
        squares = squares + jnp.where(mine, value * value, 0.0)
    for i in range(out.shape[0]):
        for k, row in enumerate((count, total, squares)):
            out[i, k : k + 1] = row


def group_sums(group, reward, copies):
    return pl.pallas_call(
        sums_kernel,
        out_shape=jax.ShapeDtypeStruct((copies, 3, LANES), f32),
        compiler_params=params(),
        cost_estimate=cost(copies * 3 * LANES, copies * 12 * LANES),
        name="group_sums",
    )(group, reward)


def stats_kernel(src, out):
    total = jnp.sum(src[...], axis=0)
    for i in range(out.shape[0]):
        out[i] = total


def stats_spread(blocks, copies):
    return pl.pallas_call(
        stats_kernel,
        out_shape=jax.ShapeDtypeStruct((copies, *blocks.shape[1:]), f32),
        compiler_params=params(),
        cost_estimate=cost(blocks.size, 8 * blocks.size),
        name="stats_spread",
    )(blocks)


def token_rows(seq_row, mask_row, group_row, reward_row, new_row, old_row, ref_row):
    onehot = (seq_row[:, None] == jnp.arange(SEQ_DEV, dtype=jnp.int32)[None, :]).astype(f32)
    maskf = mask_row.astype(f32)
    lengths = jnp.maximum(jnp.dot(maskf, onehot, precision=lax.Precision.HIGHEST), 1.0)
    tok_len = jnp.dot(onehot, lengths, precision=lax.Precision.HIGHEST)
    tok_reward = jnp.dot(onehot, reward_row, precision=lax.Precision.HIGHEST)
    tok_group = jnp.dot(onehot, group_row.astype(f32), precision=lax.Precision.HIGHEST)
    weight = maskf / tok_len
    ratio = jnp.exp(new_row - old_row)
    penalty = 0.2 * (1.0 - jnp.exp(ref_row - new_row))
    zero = jnp.zeros_like(weight)
    return jnp.stack([weight, ratio, penalty, tok_reward, tok_group, zero, zero, zero], axis=0)


def turn_kernel(pos, cot_a, cot_b, out_a, out_b):
    half, _ = out_a.shape
    rows = half // 8
    cols = pl.ds(pl.multiple_of(pos[0] * half, half), half)
    for cot, out in ((cot_a, out_a), (cot_b, out_b)):
        turned = cot[:, cols].astype(f32).T.astype(bf16)
        for y in range(4):
            out[y * rows : (y + 1) * rows, :] = turned[2 * y * rows : (2 * y + 1) * rows]
            to = pl.multiple_of((4 + (y - pos[3] + 4) % 4) * rows, rows)
            out[pl.ds(to, rows), :] = turned[(2 * y + 1) * rows : (2 * y + 2) * rows]


def turn(pos, cot_a, cot_b):
    toks, kv = cot_a.shape
    whole = lambda *shape: pl.BlockSpec(shape, lambda i, p: (0,) * len(shape))
    return pl.pallas_call(
        turn_kernel,
        out_shape=[jax.ShapeDtypeStruct((kv // 2, toks), bf16)] * 2,
        grid_spec=pltpu.PrefetchScalarGridSpec(
            num_scalar_prefetch=1,
            grid=(1,),
            in_specs=[whole(toks, kv)] * 2,
            out_specs=[whole(kv // 2, toks)] * 2,
        ),
        compiler_params=params(),
        cost_estimate=cost(4 * cot_a.size, 6 * cot_a.size),
        name="turn",
    )(pos, cot_a, cot_b)


def partial_kernel(pos, stats, tok_a, tok_b, cot_a, cot_b, hid_a, hid_b, *refs):
    outs, (hid, sems) = refs[:8], refs[8:]
    rows, blk = outs[0].shape[1:]
    copies = []
    for d in range(4):
        cols = pl.ds(pl.multiple_of((pos[1] + d) % 4 * blk, LANES), blk)
        for k, src in enumerate((hid_a, hid_b)):
            copies.append(pltpu.make_async_copy(src.at[:, cols], hid.at[d, k], sems.at[d, k]))
    for copy in copies:
        copy.start()
    sums = jnp.sum(stats[...], axis=0)
    count = jnp.maximum(sums[0:1, :], 1.0)
    mean = sums[1:2, :] / count
    spread = jnp.maximum(jnp.sqrt(jnp.maximum(sums[2:3, :] / count - mean * mean, 0.0)), 0.5)
    table = jnp.concatenate([jnp.broadcast_to(mean, (8, LANES)), jnp.broadcast_to(spread, (8, LANES))], axis=0).T
    mean, spread = table[:, 0:1], table[:, 8:9]
    delta = []
    for tok, cot in ((tok_a, cot_a), (tok_b, cot_b)):
        t = tok[...]
        group = lax.broadcasted_iota(jnp.int32, (LANES, t.shape[1]), 0).astype(f32)
        pick = group == t[4:5]
        tok_mean = jnp.sum(jnp.where(pick, mean, 0.0), axis=0, keepdims=True)
        tok_std = jnp.sum(jnp.where(pick, spread, 0.0), axis=0, keepdims=True)
        adv = (t[3:4] - tok_mean) / tok_std
        coef = t[0:1] * (-adv * t[1:2] + t[2:3])
        delta.append((cot[...].astype(f32) * coef).astype(bf16))
    for d in range(4):
        copies[2 * d].wait()
        acc = jnp.dot(delta[0], hid[d, 0], preferred_element_type=f32)
        copies[2 * d + 1].wait()
        acc = acc + jnp.dot(delta[1], hid[d, 1], preferred_element_type=f32)
        acc = acc.astype(bf16).reshape(8, rows, blk)
        outs[d][...] = acc[:4]
        for e in range(4):
            outs[4 + e][(pos[1] + d) % 4] = acc[4 + e]


def partial_product(pos, stats, tok_a, tok_b, cot_a, cot_b, hid_a, hid_b):
    toks, width = hid_a.shape
    half = cot_a.shape[0]
    blk = width // 4
    shape = (4, half // 8, blk)
    whole = lambda s: pl.BlockSpec(s, lambda i, p: (0,) * len(s))
    far = pl.BlockSpec(memory_space=pltpu.HBM)
    return pl.pallas_call(
        partial_kernel,
        out_shape=[jax.ShapeDtypeStruct(shape, bf16)] * 8,
        grid_spec=pltpu.PrefetchScalarGridSpec(
            num_scalar_prefetch=1,
            grid=(1,),
            in_specs=[whole(a.shape) for a in (stats, tok_a, tok_b, cot_a, cot_b)] + [far, far],
            out_specs=[whole(shape)] * 8,
            scratch_shapes=[pltpu.VMEM((4, 2, toks, blk), bf16), pltpu.SemaphoreType.DMA((4, 2))],
        ),
        compiler_params=params(50 * 1024 * 1024),
        cost_estimate=cost(4 * toks * width * half, 4 * toks * width + 2 * width * half),
        name="partial_product",
    )(pos, stats, tok_a, tok_b, cot_a, cot_b, hid_a, hid_b)


def sum_mid_kernel(axis, pos, *refs):
    srcs, outs = refs[:4], refs[4:]
    for d in range(4):
        k = (pos[axis] + d) % 4
        outs[d][...] = sum(src[k].astype(f32) for src in srcs).astype(bf16)


def sum_mid(pos, parts, axis):
    _, rows, width = parts[0].shape
    whole = lambda *shape: pl.BlockSpec(shape, lambda i, p: (0,) * len(shape))
    return pl.pallas_call(
        lambda *refs: sum_mid_kernel(axis, *refs),
        out_shape=[jax.ShapeDtypeStruct((rows, width), bf16)] * 4,
        grid_spec=pltpu.PrefetchScalarGridSpec(
            num_scalar_prefetch=1,
            grid=(1,),
            in_specs=[whole(4, rows, width)] * 4,
            out_specs=[whole(rows, width)] * 4,
        ),
        compiler_params=params(),
        cost_estimate=cost(16 * rows * width, 40 * rows * width),
    )(pos, *parts)


def sum_turn_kernel(*refs):
    srcs, out = refs[:8], refs[8]
    first = sum(src[...].astype(f32) for src in srcs[:4])
    second = sum(src[...].astype(f32) for src in srcs[4:])
    out[...] = jnp.concatenate([first, second], axis=0).T.astype(bf16)


def sum_turn(first, second):
    rows, width = first[0].shape
    return pl.pallas_call(
        sum_turn_kernel,
        out_shape=jax.ShapeDtypeStruct((width, 2 * rows), bf16),
        compiler_params=params(),
        cost_estimate=cost(8 * rows * width, 20 * rows * width),
        name="sum_turn",
    )(*first, *second)


def sum_spread_kernel(src, out):
    total = jnp.sum(src[...].astype(f32), axis=0).astype(bf16)
    for i in range(out.shape[0]):
        out[i] = total


def sum_spread(blocks, copies):
    n, rows, width = blocks.shape
    return pl.pallas_call(
        sum_spread_kernel,
        out_shape=jax.ShapeDtypeStruct((copies, rows, width), bf16),
        compiler_params=params(),
        cost_estimate=cost(n * rows * width, 4 * n * rows * width),
        name="sum_spread",
    )(blocks)


def send_kernel(pos, grad, blocks):
    g = grad[...].astype(f32)
    s = jnp.sum(g * g, axis=(0, 1, 2))
    s = jnp.sum(jnp.sum(s, axis=0, keepdims=True), axis=1, keepdims=True)
    high = s.astype(bf16).astype(f32)
    mid = (s - high).astype(bf16).astype(f32)
    low = s - high - mid
    rows = grad.shape[3]
    row = lax.broadcasted_iota(jnp.int32, (8, 2 * HEAD), 0)
    tail = jnp.where(row == 0, high, jnp.where(row == 1, mid, jnp.where(row == 2, low, 0.0))).astype(bf16)
    for h in range(KV_HEADS):
        for i in range(2):
            for j in range(2):
                for kv in range(2):
                    blocks[i, h, j, :rows, kv * HEAD : (kv + 1) * HEAD] = grad[pos[0], h, kv]
                blocks[i, h, j, rows:, :] = tail


def send_blocks(pos, grad):
    rows = grad.shape[3]
    whole = lambda s: pl.BlockSpec(s, lambda i, p: (0,) * len(s))
    shape = (2, KV_HEADS, 2, rows + 8, 2 * HEAD)
    return pl.pallas_call(
        send_kernel,
        out_shape=jax.ShapeDtypeStruct(shape, bf16),
        grid_spec=pltpu.PrefetchScalarGridSpec(
            num_scalar_prefetch=1, grid=(1,), in_specs=[whole(grad.shape)], out_specs=whole(shape)
        ),
        compiler_params=params(60 * 1024 * 1024),
        cost_estimate=cost(4 * grad.size, 8 * grad.size),
        name="send_blocks",
    )(pos, grad)


def step_size(squares, entries):
    s = jnp.sum(squares[...].astype(f32), axis=0)[:, 0:1]
    total = s[0:1] + s[1:2] + s[2:3]
    return 0.5 / jnp.sqrt(total / entries + 1e-06)


def update_kernel(entries, squares, grad, master, new):
    zl, ny, _, rows, width = grad.shape
    step = step_size(squares, entries)
    for kv in range(2):
        for y in range(ny):
            for z in range(zl):
                r = slice(z * rows, (z + 1) * rows)
                c = slice((kv * ny + y) * width, (kv * ny + y + 1) * width)
                new[r, c] = master[0, r, c] - grad[z, y, kv].astype(f32) * step


def update(received, grad, master, entries):
    _, rows, kv = master.shape
    return pl.pallas_call(
        lambda *refs: update_kernel(entries, *refs),
        out_shape=jax.ShapeDtypeStruct((rows, kv), f32),
        grid=(1,),
        in_specs=[
            pl.BlockSpec((received.shape[0], 8, LANES), lambda i: (0, rows // 16, 0)),
            pl.BlockSpec(grad.shape, lambda i: (0, 0, 0, 0, 0)),
            pl.BlockSpec((1, rows, kv), lambda i: (0, 0, 0)),
        ],
        out_specs=pl.BlockSpec((rows, kv), lambda i: (0, 0)),
        compiler_params=params(),
        cost_estimate=cost(4 * rows * kv, 10 * rows * kv),
        name="update",
    )(received, grad, master)


def rest_kernel(pos, *refs):
    masters, outs = refs[:8], refs[8:]
    for d in range(4):
        for kv in range(2):
            outs[d][0, :, :, kv * HEAD : (kv + 1) * HEAD] = masters[2 * d + kv][...].astype(bf16)


def rest_blocks(pos, master):
    layers, rows, kv = master.shape
    half = rows // 2

    def spec(d, k):
        return pl.BlockSpec(
            (layers, half, HEAD),
            lambda xl, p: (0, p[0], k * KV_HEADS + xl * 2 + ((p[2] + d) % 4) // 2),
        )

    shape = (2, layers, half, 2 * HEAD)
    return pl.pallas_call(
        rest_kernel,
        out_shape=[jax.ShapeDtypeStruct(shape, bf16)] * 4,
        grid_spec=pltpu.PrefetchScalarGridSpec(
            num_scalar_prefetch=1,
            grid=(2,),
            in_specs=[spec(d, k) for d in range(4) for k in range(2)],
            out_specs=[pl.BlockSpec((1, *shape[1:]), lambda xl, p: (xl, 0, 0, 0))] * 4,
        ),
        compiler_params=params(),
        cost_estimate=cost(layers * rows * kv, 12 * rows * kv),
        name="rest_blocks",
    )(pos, *([master] * 8))


def regroup_kernel(pos, *refs):
    parts, (same, cross), sems = refs[:4], refs[4:6], refs[6]
    xl = pos[1] % 2
    copies = []
    for d in range(4):
        copies.append(pltpu.make_async_copy(parts[d].at[xl], same.at[d], sems.at[2 * d]))
        copies.append(pltpu.make_async_copy(parts[d].at[1 - xl], cross.at[d], sems.at[2 * d + 1]))
    for copy in copies:
        copy.start()
    for copy in copies:
        copy.wait()


def regroup(pos, parts):
    shape = (4, *parts[0].shape[1:])
    whole = lambda s: pl.BlockSpec(s, lambda i, p: (0,) * len(s))
    return pl.pallas_call(
        regroup_kernel,
        out_shape=[jax.ShapeDtypeStruct(shape, bf16)] * 2,
        grid_spec=pltpu.PrefetchScalarGridSpec(
            num_scalar_prefetch=1,
            grid=(1,),
            in_specs=[pl.BlockSpec(memory_space=pltpu.HBM)] * 4,
            out_specs=[whole(shape)] * 2,
            scratch_shapes=[pltpu.SemaphoreType.DMA((8,))],
        ),
        compiler_params=params(),
        cost_estimate=cost(parts[0].size, 16 * parts[0].size),
        name="regroup",
    )(pos, *parts)


def place_rest_kernel(pos, *refs):
    srcs, out = refs[:8], refs[8]
    zh, core = pos[2], pos[0]
    for dx in range(4):

        @pl.when(pl.program_id(1) == dx)
        def _():
            for w in range(2):
                for dz in range(4):
                    out[0, 0, (zh - dz + 4) % 4, (core + w) % 2] = srcs[4 * w + dx][dz, 0]


def place_rest(pos, own, other, layers):
    _, count, half, width = own[0].shape
    src = pl.BlockSpec((4, 1, half, width), lambda l, d, p: (0, 1 + l, 0, 0))
    return pl.pallas_call(
        place_rest_kernel,
        out_shape=jax.ShapeDtypeStruct((layers, 4, 4, 2, half, width), bf16),
        grid_spec=pltpu.PrefetchScalarGridSpec(
            num_scalar_prefetch=1,
            grid=(count - 1, 4),
            in_specs=[src] * 8,
            out_specs=pl.BlockSpec(
                (1, 1, 4, 2, half, width), lambda l, d, p: (1 + l, (p[1] - d + 4) % 4, 0, 0, 0, 0)
            ),
        ),
        compiler_params=params(58 * 1024 * 1024),
        cost_estimate=cost(own[0].size, 32 * own[0].size),
        name="place_rest",
    )(pos, *own, *other)


def finish_kernel(entries, pos, squares, grad_a, grad_b, *refs):
    masters, out = refs[:8], refs[9]
    zh, core = pos[2], pos[0]
    step = step_size(squares, entries)
    half = out.shape[4]
    for dx in range(4):

        @pl.when(pl.program_id(0) == dx)
        def _():
            for w in range(2):
                grad = (grad_a, grad_b)[w]
                for dz in range(4):
                    k = (zh - dz + 4) % 4
                    value = masters[4 * w + dx][dz, 0].astype(f32) - grad[k, :half].astype(f32) * step
                    out[0, 0, k, (core + w) % 2] = value.astype(bf16)


def finish(pos, grad_a, grad_b, own, other, into, entries):
    n, padded, width = grad_a.shape
    half = padded - 8
    grad = pl.BlockSpec((4, padded, width), lambda d, p: ((p[1] - d + 4) % 4, 0, 0))
    src = pl.BlockSpec((4, 1, half, width), lambda d, p: (0, 0, 0, 0))
    return pl.pallas_call(
        lambda *refs: finish_kernel(entries, *refs),
        out_shape=jax.ShapeDtypeStruct(into.shape, bf16),
        grid_spec=pltpu.PrefetchScalarGridSpec(
            num_scalar_prefetch=1,
            grid=(4,),
            in_specs=[pl.BlockSpec((n, 8, LANES), lambda d, p: (0, half // 8, 0)), grad, grad]
            + [src] * 8
            + [pl.BlockSpec(memory_space=pl.ANY)],
            out_specs=pl.BlockSpec(
                (1, 1, 4, 2, half, width), lambda d, p: (0, (p[1] - d + 4) % 4, 0, 0, 0, 0)
            ),
        ),
        input_output_aliases={12: 0},
        compiler_params=params(),
        cost_estimate=cost(8 * grad_a.size, 24 * grad_a.size),
        name="finish",
    )(pos, grad_a, grad_a, grad_b, *own, *other, into)


def per_device(
    hidden,
    cotangent,
    seq_ids,
    response_mask,
    group_ids,
    rewards,
    new_logp,
    old_logp,
    ref_logp,
    master,
):
    n_y, n_z = lax.axis_size("y"), lax.axis_size(("zh", "zl"))
    n_shard = lax.axis_size(SHARD)
    layers, rows, kv = master.shape
    pos = jnp.stack([lax.axis_index(a).astype(jnp.int32) for a in ("c", "x", "zh", "y")])

    first, second = ("x", "y"), ("zh", "zl", "c")
    stats = exchanged(group_sums(group_ids, rewards, lax.axis_size(first)), first)
    stats = stats_spread(stats, lax.axis_size(second))
    stats = exchanged(stats, second)

    hidden_b = swapped(hidden)
    cotangent_b = swapped(cotangent)
    tok = token_rows(
        seq_ids[0], response_mask[0], group_ids[0], rewards[0], new_logp[0], old_logp[0], ref_logp[0]
    )
    tok_b = swapped(tok)

    turned = turn(pos, cotangent, cotangent_b)
    partial = partial_product(pos, stats, tok, tok_b, *turned, hidden, hidden_b)
    to_x = spread_out(partial[:4], "x")
    to_y = spread_out(partial[4:], "y")
    to_x = sum_mid(pos, to_x, 3)
    to_x = spread_out(to_x, "y")
    to_y = sum_mid(pos, to_y, 1)
    to_y = spread_out(to_y, "x")
    part = sum_turn(to_x, to_y)

    parts = rest_blocks(pos, master)
    parts = spread_out(parts, "zh")
    same, cross = regroup(pos, parts)
    rest = spread_out([same, cross, same, cross], "x")
    part = part.reshape(n_z, part.shape[0] // n_z, part.shape[1])
    zl = lax.axis_size("zl")
    part = exchanged(part, ("zh", "zl"))
    grad = exchanged(sum_spread(part, zl * n_y * 2), REP)
    grad = grad.reshape(zl, n_y, 2, *grad.shape[1:])
    first = send_blocks(pos, grad)
    first = exchanged(first.reshape(n_shard, *first.shape[3:]), SHARD)

    other = [swapped(r) for r in rest]
    out = place_rest(pos, rest, other, layers)
    entries = hidden.shape[1] * kv
    first_b = swapped(first)
    new_master = update(first, grad, master, entries)
    out = finish(pos, first, first_b, rest, other, out, entries)
    return (new_master, out.reshape(layers, n_shard * rows, 2 * HEAD))


def solution(mesh):
    split = Mesh(mesh.devices.reshape(2, 4, 2, 4, 4), REP + SHARD)
    row = P(REP + SHARD, None)
    return jax.shard_map(
        per_device,
        mesh=split,
        in_specs=(row,) * 9 + (P(None, SHARD, None),),
        out_specs=(P(SHARD, None), P(None, None, SHARD)),
        check_vma=False,
    )
```

```python
import jax
import jax.numpy as jnp
from jax import lax
from jax.experimental import pallas as pl
from jax.experimental.pallas import tpu as pltpu
from jax.sharding import Mesh
from jax.sharding import PartitionSpec as P

HEAD = 128
KV_HEADS = 4
SEQ_DEV = 4
LANES = 128
REP = ("zl", "y", "c")
SHARD = ("x", "zh")
VMEM_LIMIT = 24 * 1024 * 1024
f32 = jnp.float32
bf16 = jnp.bfloat16


def swapped(value):
    return lax.ppermute(value, "c", [(0, 1), (1, 0)])


def shifted(value, axis, by):
    n = lax.axis_size(axis)
    return lax.ppermute(value, axis, [(i, (i + by) % n) for i in range(n)])


def spread_out(blocks, axis):
    return [blocks[0]] + [shifted(blocks[d], axis, d) for d in range(1, 4)]


def exchanged(blocks, axis):
    return lax.all_to_all(blocks, axis, split_axis=0, concat_axis=0, tiled=True)


def params(limit=VMEM_LIMIT):
    return pltpu.CompilerParams(vmem_limit_bytes=limit)


def cost(flops, nbytes):
    return pl.CostEstimate(flops=flops, bytes_accessed=nbytes, transcendentals=0)


def sums_kernel(group, reward, out):
    lane = lax.broadcasted_iota(jnp.int32, (1, LANES), 1)
    count = total = squares = jnp.zeros((1, LANES), f32)
    for k in range(SEQ_DEV):
        value = reward[:, k : k + 1]
        mine = lane == group[:, k : k + 1]
        count = count + jnp.where(mine, 1.0, 0.0)
        total = total + jnp.where(mine, value, 0.0)
        squares = squares + jnp.where(mine, value * value, 0.0)
    for i in range(out.shape[0]):
        for k, row in enumerate((count, total, squares)):
            out[i, k : k + 1] = row


def group_sums(group, reward, copies):
    return pl.pallas_call(
        sums_kernel,
        out_shape=jax.ShapeDtypeStruct((copies, 3, LANES), f32),
        compiler_params=params(),
        cost_estimate=cost(copies * 3 * LANES, copies * 12 * LANES),
        name="group_sums",
    )(group, reward)


def stats_kernel(src, out):
    total = jnp.sum(src[...], axis=0)
    for i in range(out.shape[0]):
        out[i] = total


def stats_spread(blocks, copies):
    return pl.pallas_call(
        stats_kernel,
        out_shape=jax.ShapeDtypeStruct((copies, *blocks.shape[1:]), f32),
        compiler_params=params(),
        cost_estimate=cost(blocks.size, 8 * blocks.size),
        name="stats_spread",
    )(blocks)


def token_rows(seq_row, mask_row, group_row, reward_row, new_row, old_row, ref_row):
    onehot = (seq_row[:, None] == jnp.arange(SEQ_DEV, dtype=jnp.int32)[None, :]).astype(f32)
    maskf = mask_row.astype(f32)
    lengths = jnp.maximum(jnp.dot(maskf, onehot, precision=lax.Precision.HIGHEST), 1.0)
    tok_len = jnp.dot(onehot, lengths, precision=lax.Precision.HIGHEST)
    tok_reward = jnp.dot(onehot, reward_row, precision=lax.Precision.HIGHEST)
    tok_group = jnp.dot(onehot, group_row.astype(f32), precision=lax.Precision.HIGHEST)
    weight = maskf / tok_len
    ratio = jnp.exp(new_row - old_row)
    penalty = 0.2 * (1.0 - jnp.exp(ref_row - new_row))
    zero = jnp.zeros_like(weight)
    return jnp.stack([weight, ratio, penalty, tok_reward, tok_group, zero, zero, zero], axis=0)


def turn_kernel(pos, cot_a, cot_b, out_a, out_b):
    half, _ = out_a.shape
    rows = half // 8
    cols = pl.ds(pl.multiple_of(pos[0] * half, half), half)
    for cot, out in ((cot_a, out_a), (cot_b, out_b)):
        turned = cot[:, cols].astype(f32).T.astype(bf16)
        for y in range(4):
            out[y * rows : (y + 1) * rows, :] = turned[2 * y * rows : (2 * y + 1) * rows]
            to = pl.multiple_of((4 + (y - pos[3] + 4) % 4) * rows, rows)
            out[pl.ds(to, rows), :] = turned[(2 * y + 1) * rows : (2 * y + 2) * rows]


def turn(pos, cot_a, cot_b):
    toks, kv = cot_a.shape
    whole = lambda *shape: pl.BlockSpec(shape, lambda i, p: (0,) * len(shape))
    return pl.pallas_call(
        turn_kernel,
        out_shape=[jax.ShapeDtypeStruct((kv // 2, toks), bf16)] * 2,
        grid_spec=pltpu.PrefetchScalarGridSpec(
            num_scalar_prefetch=1,
            grid=(1,),
            in_specs=[whole(toks, kv)] * 2,
            out_specs=[whole(kv // 2, toks)] * 2,
        ),
        compiler_params=params(),
        cost_estimate=cost(4 * cot_a.size, 6 * cot_a.size),
        name="turn",
    )(pos, cot_a, cot_b)


def partial_kernel(pos, stats, tok_a, tok_b, cot_a, cot_b, hid_a, hid_b, *refs):
    outs, (hid, sems) = refs[:8], refs[8:]
    rows, blk = outs[0].shape[1:]
    copies = []
    for d in range(4):
        cols = pl.ds(pl.multiple_of((pos[1] + d) % 4 * blk, LANES), blk)
        for k, src in enumerate((hid_a, hid_b)):
            copies.append(pltpu.make_async_copy(src.at[:, cols], hid.at[d, k], sems.at[d, k]))
    for copy in copies:
        copy.start()
    sums = jnp.sum(stats[...], axis=0)
    count = jnp.maximum(sums[0:1, :], 1.0)
    mean = sums[1:2, :] / count
    spread = jnp.maximum(jnp.sqrt(jnp.maximum(sums[2:3, :] / count - mean * mean, 0.0)), 0.5)
    table = jnp.concatenate([jnp.broadcast_to(mean, (8, LANES)), jnp.broadcast_to(spread, (8, LANES))], axis=0).T
    mean, spread = table[:, 0:1], table[:, 8:9]
    delta = []
    for tok, cot in ((tok_a, cot_a), (tok_b, cot_b)):
        t = tok[...]
        group = lax.broadcasted_iota(jnp.int32, (LANES, t.shape[1]), 0).astype(f32)
        pick = group == t[4:5]
        tok_mean = jnp.sum(jnp.where(pick, mean, 0.0), axis=0, keepdims=True)
        tok_std = jnp.sum(jnp.where(pick, spread, 0.0), axis=0, keepdims=True)
        adv = (t[3:4] - tok_mean) / tok_std
        coef = t[0:1] * (-adv * t[1:2] + t[2:3])
        delta.append((cot[...].astype(f32) * coef).astype(bf16))
    for d in range(4):
        copies[2 * d].wait()
        acc = jnp.dot(delta[0], hid[d, 0], preferred_element_type=f32)
        copies[2 * d + 1].wait()
        acc = acc + jnp.dot(delta[1], hid[d, 1], preferred_element_type=f32)
        acc = acc.astype(bf16).reshape(8, rows, blk)
        outs[d][...] = acc[:4]
        for e in range(4):
            outs[4 + e][(pos[1] + d) % 4] = acc[4 + e]


def partial_product(pos, stats, tok_a, tok_b, cot_a, cot_b, hid_a, hid_b):
    toks, width = hid_a.shape
    half = cot_a.shape[0]
    blk = width // 4
    shape = (4, half // 8, blk)
    whole = lambda s: pl.BlockSpec(s, lambda i, p: (0,) * len(s))
    far = pl.BlockSpec(memory_space=pltpu.HBM)
    return pl.pallas_call(
        partial_kernel,
        out_shape=[jax.ShapeDtypeStruct(shape, bf16)] * 8,
        grid_spec=pltpu.PrefetchScalarGridSpec(
            num_scalar_prefetch=1,
            grid=(1,),
            in_specs=[whole(a.shape) for a in (stats, tok_a, tok_b, cot_a, cot_b)] + [far, far],
            out_specs=[whole(shape)] * 8,
            scratch_shapes=[pltpu.VMEM((4, 2, toks, blk), bf16), pltpu.SemaphoreType.DMA((4, 2))],
        ),
        compiler_params=params(50 * 1024 * 1024),
        cost_estimate=cost(4 * toks * width * half, 4 * toks * width + 2 * width * half),
        name="partial_product",
    )(pos, stats, tok_a, tok_b, cot_a, cot_b, hid_a, hid_b)


def sum_mid_kernel(axis, pos, *refs):
    srcs, outs = refs[:4], refs[4:]
    for d in range(4):
        k = (pos[axis] + d) % 4
        outs[d][...] = sum(src[k].astype(f32) for src in srcs).astype(bf16)


def sum_mid(pos, parts, axis):
    _, rows, width = parts[0].shape
    whole = lambda *shape: pl.BlockSpec(shape, lambda i, p: (0,) * len(shape))
    return pl.pallas_call(
        lambda *refs: sum_mid_kernel(axis, *refs),
        out_shape=[jax.ShapeDtypeStruct((rows, width), bf16)] * 4,
        grid_spec=pltpu.PrefetchScalarGridSpec(
            num_scalar_prefetch=1,
            grid=(1,),
            in_specs=[whole(4, rows, width)] * 4,
            out_specs=[whole(rows, width)] * 4,
        ),
        compiler_params=params(),
        cost_estimate=cost(16 * rows * width, 40 * rows * width),
    )(pos, *parts)


def sum_turn_kernel(*refs):
    srcs, out = refs[:8], refs[8]
    first = sum(src[...].astype(f32) for src in srcs[:4])
    second = sum(src[...].astype(f32) for src in srcs[4:])
    out[...] = jnp.concatenate([first, second], axis=0).T.astype(bf16)


def sum_turn(first, second):
    rows, width = first[0].shape
    return pl.pallas_call(
        sum_turn_kernel,
        out_shape=jax.ShapeDtypeStruct((width, 2 * rows), bf16),
        compiler_params=params(),
        cost_estimate=cost(8 * rows * width, 20 * rows * width),
        name="sum_turn",
    )(*first, *second)


def sum_spread_kernel(src, out):
    total = jnp.sum(src[...].astype(f32), axis=0).astype(bf16)
    for i in range(out.shape[0]):
        out[i] = total


def sum_spread(blocks, copies):
    n, rows, width = blocks.shape
    return pl.pallas_call(
        sum_spread_kernel,
        out_shape=jax.ShapeDtypeStruct((copies, rows, width), bf16),
        compiler_params=params(),
        cost_estimate=cost(n * rows * width, 4 * n * rows * width),
        name="sum_spread",
    )(blocks)


def send_kernel(pos, grad, blocks):
    g = grad[...].astype(f32)
    s = jnp.sum(g * g, axis=(0, 1, 2))
    s = jnp.sum(jnp.sum(s, axis=0, keepdims=True), axis=1, keepdims=True)
    high = s.astype(bf16).astype(f32)
    mid = (s - high).astype(bf16).astype(f32)
    low = s - high - mid
    rows = grad.shape[3]
    row = lax.broadcasted_iota(jnp.int32, (8, 2 * HEAD), 0)
    tail = jnp.where(row == 0, high, jnp.where(row == 1, mid, jnp.where(row == 2, low, 0.0))).astype(bf16)
    for h in range(KV_HEADS):
        for i in range(2):
            for j in range(2):
                for kv in range(2):
                    blocks[i, h, j, :rows, kv * HEAD : (kv + 1) * HEAD] = grad[pos[0], h, kv]
                blocks[i, h, j, rows:, :] = tail


def send_blocks(pos, grad):
    rows = grad.shape[3]
    whole = lambda s: pl.BlockSpec(s, lambda i, p: (0,) * len(s))
    shape = (2, KV_HEADS, 2, rows + 8, 2 * HEAD)
    return pl.pallas_call(
        send_kernel,
        out_shape=jax.ShapeDtypeStruct(shape, bf16),
        grid_spec=pltpu.PrefetchScalarGridSpec(
            num_scalar_prefetch=1, grid=(1,), in_specs=[whole(grad.shape)], out_specs=whole(shape)
        ),
        compiler_params=params(60 * 1024 * 1024),
        cost_estimate=cost(4 * grad.size, 8 * grad.size),
        name="send_blocks",
    )(pos, grad)


def step_size(squares, entries):
    s = jnp.sum(squares[...].astype(f32), axis=0)[:, 0:1]
    total = s[0:1] + s[1:2] + s[2:3]
    return 0.5 / jnp.sqrt(total / entries + 1e-06)


def update_kernel(entries, squares, grad, master, new):
    zl, ny, _, rows, width = grad.shape
    step = step_size(squares, entries)
    for kv in range(2):
        for y in range(ny):
            for z in range(zl):
                r = slice(z * rows, (z + 1) * rows)
                c = slice((kv * ny + y) * width, (kv * ny + y + 1) * width)
                new[r, c] = master[0, r, c] - grad[z, y, kv].astype(f32) * step


def update(received, grad, master, entries):
    _, rows, kv = master.shape
    return pl.pallas_call(
        lambda *refs: update_kernel(entries, *refs),
        out_shape=jax.ShapeDtypeStruct((rows, kv), f32),
        grid=(1,),
        in_specs=[
            pl.BlockSpec((received.shape[0], 8, LANES), lambda i: (0, rows // 16, 0)),
            pl.BlockSpec(grad.shape, lambda i: (0, 0, 0, 0, 0)),
            pl.BlockSpec((1, rows, kv), lambda i: (0, 0, 0)),
        ],
        out_specs=pl.BlockSpec((rows, kv), lambda i: (0, 0)),
        compiler_params=params(),
        cost_estimate=cost(4 * rows * kv, 10 * rows * kv),
        name="update",
    )(received, grad, master)


def rest_kernel(pos, *refs):
    masters, outs = refs[:8], refs[8:]
    for d in range(4):
        for kv in range(2):
            outs[d][0, :, :, kv * HEAD : (kv + 1) * HEAD] = masters[2 * d + kv][...].astype(bf16)


def rest_blocks(pos, master):
    layers, rows, kv = master.shape
    half = rows // 2

    def spec(d, k):
        return pl.BlockSpec(
            (layers, half, HEAD),
            lambda xl, p: (0, p[0], k * KV_HEADS + xl * 2 + ((p[2] + d) % 4) // 2),
        )

    shape = (2, layers, half, 2 * HEAD)
    return pl.pallas_call(
        rest_kernel,
        out_shape=[jax.ShapeDtypeStruct(shape, bf16)] * 4,
        grid_spec=pltpu.PrefetchScalarGridSpec(
            num_scalar_prefetch=1,
            grid=(2,),
            in_specs=[spec(d, k) for d in range(4) for k in range(2)],
            out_specs=[pl.BlockSpec((1, *shape[1:]), lambda xl, p: (xl, 0, 0, 0))] * 4,
        ),
        compiler_params=params(),
        cost_estimate=cost(layers * rows * kv, 12 * rows * kv),
        name="rest_blocks",
    )(pos, *([master] * 8))


def regroup_kernel(pos, *refs):
    parts, (same, cross), sems = refs[:4], refs[4:6], refs[6]
    xl = pos[1] % 2
    copies = []
    for d in range(4):
        copies.append(pltpu.make_async_copy(parts[d].at[xl], same.at[d], sems.at[2 * d]))
        copies.append(pltpu.make_async_copy(parts[d].at[1 - xl], cross.at[d], sems.at[2 * d + 1]))
    for copy in copies:
        copy.start()
    for copy in copies:
        copy.wait()


def regroup(pos, parts):
    shape = (4, *parts[0].shape[1:])
    whole = lambda s: pl.BlockSpec(s, lambda i, p: (0,) * len(s))
    return pl.pallas_call(
        regroup_kernel,
        out_shape=[jax.ShapeDtypeStruct(shape, bf16)] * 2,
        grid_spec=pltpu.PrefetchScalarGridSpec(
            num_scalar_prefetch=1,
            grid=(1,),
            in_specs=[pl.BlockSpec(memory_space=pltpu.HBM)] * 4,
            out_specs=[whole(shape)] * 2,
            scratch_shapes=[pltpu.SemaphoreType.DMA((8,))],
        ),
        compiler_params=params(),
        cost_estimate=cost(parts[0].size, 16 * parts[0].size),
        name="regroup",
    )(pos, *parts)


def place_rest_kernel(pos, own, other, *refs):
    out = refs[-1]
    zh, core = pos[2], pos[0]
    for w, src in enumerate((own, other)):
        for dz in range(4):
            out[0, 0, (zh - dz + 4) % 4, (core + w) % 2] = src[dz, 0]


def place_rest(pos, own, other, dx, into=None):
    _, layers, half, width = own.shape
    src = pl.BlockSpec((4, 1, half, width), lambda l, p: (0, 1 + l, 0, 0))
    keep = [] if into is None else [into]
    return pl.pallas_call(
        place_rest_kernel,
        out_shape=jax.ShapeDtypeStruct((layers, 4, 4, 2, half, width), bf16),
        grid_spec=pltpu.PrefetchScalarGridSpec(
            num_scalar_prefetch=1,
            grid=(layers - 1,),
            in_specs=[src, src] + [pl.BlockSpec(memory_space=pl.ANY)] * len(keep),
            out_specs=pl.BlockSpec(
                (1, 1, 4, 2, half, width), lambda l, p: (1 + l, (p[1] - dx + 4) % 4, 0, 0, 0, 0)
            ),
        ),
        input_output_aliases={3: 0} if keep else {},
        compiler_params=params(58 * 1024 * 1024),
        cost_estimate=cost(own.size, 8 * own.size),
    )(pos, own, other, *keep)


def finish_kernel(entries, pos, squares, grad_a, grad_b, *refs):
    masters, out = refs[:8], refs[9]
    zh, core = pos[2], pos[0]
    step = step_size(squares, entries)
    half = out.shape[4]
    for dx in range(4):

        @pl.when(pl.program_id(0) == dx)
        def _():
            for w in range(2):
                grad = (grad_a, grad_b)[w]
                for dz in range(4):
                    k = (zh - dz + 4) % 4
                    value = masters[4 * w + dx][dz, 0].astype(f32) - grad[k, :half].astype(f32) * step
                    out[0, 0, k, (core + w) % 2] = value.astype(bf16)


def finish(pos, grad_a, grad_b, own, other, into, entries):
    n, padded, width = grad_a.shape
    half = padded - 8
    grad = pl.BlockSpec((4, padded, width), lambda d, p: ((p[1] - d + 4) % 4, 0, 0))
    src = pl.BlockSpec((4, 1, half, width), lambda d, p: (0, 0, 0, 0))
    return pl.pallas_call(
        lambda *refs: finish_kernel(entries, *refs),
        out_shape=jax.ShapeDtypeStruct(into.shape, bf16),
        grid_spec=pltpu.PrefetchScalarGridSpec(
            num_scalar_prefetch=1,
            grid=(4,),
            in_specs=[pl.BlockSpec((n, 8, LANES), lambda d, p: (0, half // 8, 0)), grad, grad]
            + [src] * 8
            + [pl.BlockSpec(memory_space=pl.ANY)],
            out_specs=pl.BlockSpec(
                (1, 1, 4, 2, half, width), lambda d, p: (0, (p[1] - d + 4) % 4, 0, 0, 0, 0)
            ),
        ),
        input_output_aliases={12: 0},
        compiler_params=params(),
        cost_estimate=cost(8 * grad_a.size, 24 * grad_a.size),
        name="finish",
    )(pos, grad_a, grad_a, grad_b, *own, *other, into)


def per_device(
    hidden,
    cotangent,
    seq_ids,
    response_mask,
    group_ids,
    rewards,
    new_logp,
    old_logp,
    ref_logp,
    master,
):
    n_y, n_z = lax.axis_size("y"), lax.axis_size(("zh", "zl"))
    n_shard = lax.axis_size(SHARD)
    layers, rows, kv = master.shape
    pos = jnp.stack([lax.axis_index(a).astype(jnp.int32) for a in ("c", "x", "zh", "y")])

    first, second = ("x", "y"), ("zh", "zl", "c")
    stats = exchanged(group_sums(group_ids, rewards, lax.axis_size(first)), first)
    stats = stats_spread(stats, lax.axis_size(second))
    stats = exchanged(stats, second)

    hidden_b = swapped(hidden)
    cotangent_b = swapped(cotangent)
    tok = token_rows(
        seq_ids[0], response_mask[0], group_ids[0], rewards[0], new_logp[0], old_logp[0], ref_logp[0]
    )
    tok_b = swapped(tok)

    turned = turn(pos, cotangent, cotangent_b)
    partial = partial_product(pos, stats, tok, tok_b, *turned, hidden, hidden_b)
    to_x = spread_out(partial[:4], "x")
    to_y = spread_out(partial[4:], "y")
    to_x = sum_mid(pos, to_x, 3)
    to_x = spread_out(to_x, "y")
    to_y = sum_mid(pos, to_y, 1)
    to_y = spread_out(to_y, "x")
    part = sum_turn(to_x, to_y)

    parts = rest_blocks(pos, master)
    parts = spread_out(parts, "zh")
    same, cross = regroup(pos, parts)
    rest = [same]
    for d in range(1, 4):
        rest.append(shifted(cross if d % 2 else same, "x", d))
    part = part.reshape(n_z, part.shape[0] // n_z, part.shape[1])
    zl = lax.axis_size("zl")
    part = exchanged(part, ("zh", "zl"))
    grad = exchanged(sum_spread(part, zl * n_y * 2), REP)
    grad = grad.reshape(zl, n_y, 2, *grad.shape[1:])
    first = send_blocks(pos, grad)
    first = exchanged(first.reshape(n_shard, *first.shape[3:]), SHARD)

    other = [swapped(r) for r in rest]
    out = None
    for d in (0, 2, 1, 3):
        out = place_rest(pos, rest[d], other[d], d, out)
    entries = hidden.shape[1] * kv
    first_b = swapped(first)
    new_master = update(first, grad, master, entries)
    out = finish(pos, first, first_b, rest, other, out, entries)
    return (new_master, out.reshape(layers, n_shard * rows, 2 * HEAD))


def solution(mesh):
    split = Mesh(mesh.devices.reshape(2, 4, 2, 4, 4), REP + SHARD)
    row = P(REP + SHARD, None)
    return jax.shard_map(
        per_device,
        mesh=split,
        in_specs=(row,) * 9 + (P(None, SHARD, None),),
        out_specs=(P(SHARD, None), P(None, None, SHARD)),
        check_vma=False,
    )
```

```python
import jax
import jax.numpy as jnp
from jax import lax
from jax.experimental import pallas as pl
from jax.experimental.pallas import tpu as pltpu
from jax.sharding import Mesh
from jax.sharding import PartitionSpec as P

HEAD = 128
KV_HEADS = 4
SEQ_DEV = 4
LANES = 128
REP = ("zl", "y", "c")
SHARD = ("x", "zh")
VMEM_LIMIT = 24 * 1024 * 1024
f32 = jnp.float32
bf16 = jnp.bfloat16


def swapped(value):
    return lax.ppermute(value, "c", [(0, 1), (1, 0)])


def shifted(value, axis, by):
    n = lax.axis_size(axis)
    return lax.ppermute(value, axis, [(i, (i + by) % n) for i in range(n)])


def spread_out(blocks, axis):
    return [blocks[0]] + [shifted(blocks[d], axis, d) for d in range(1, 4)]


def exchanged(blocks, axis):
    return lax.all_to_all(blocks, axis, split_axis=0, concat_axis=0, tiled=True)


def params(limit=VMEM_LIMIT):
    return pltpu.CompilerParams(vmem_limit_bytes=limit)


def cost(flops, nbytes):
    return pl.CostEstimate(flops=flops, bytes_accessed=nbytes, transcendentals=0)


def sums_kernel(group, reward, out):
    lane = lax.broadcasted_iota(jnp.int32, (1, LANES), 1)
    count = total = squares = jnp.zeros((1, LANES), f32)
    for k in range(SEQ_DEV):
        value = reward[:, k : k + 1]
        mine = lane == group[:, k : k + 1]
        count = count + jnp.where(mine, 1.0, 0.0)
        total = total + jnp.where(mine, value, 0.0)
        squares = squares + jnp.where(mine, value * value, 0.0)
    for i in range(out.shape[0]):
        for k, row in enumerate((count, total, squares)):
            out[i, k : k + 1] = row


def group_sums(group, reward, copies):
    return pl.pallas_call(
        sums_kernel,
        out_shape=jax.ShapeDtypeStruct((copies, 3, LANES), f32),
        compiler_params=params(),
        cost_estimate=cost(copies * 3 * LANES, copies * 12 * LANES),
        name="group_sums",
    )(group, reward)


def stats_kernel(src, out):
    total = jnp.sum(src[...], axis=0)
    for i in range(out.shape[0]):
        out[i] = total


def stats_spread(blocks, copies):
    return pl.pallas_call(
        stats_kernel,
        out_shape=jax.ShapeDtypeStruct((copies, *blocks.shape[1:]), f32),
        compiler_params=params(),
        cost_estimate=cost(blocks.size, 8 * blocks.size),
        name="stats_spread",
    )(blocks)


def token_rows(seq_row, mask_row, group_row, reward_row, new_row, old_row, ref_row):
    onehot = (seq_row[:, None] == jnp.arange(SEQ_DEV, dtype=jnp.int32)[None, :]).astype(f32)
    maskf = mask_row.astype(f32)
    lengths = jnp.maximum(jnp.dot(maskf, onehot, precision=lax.Precision.HIGHEST), 1.0)
    tok_len = jnp.dot(onehot, lengths, precision=lax.Precision.HIGHEST)
    tok_reward = jnp.dot(onehot, reward_row, precision=lax.Precision.HIGHEST)
    tok_group = jnp.dot(onehot, group_row.astype(f32), precision=lax.Precision.HIGHEST)
    weight = maskf / tok_len
    ratio = jnp.exp(new_row - old_row)
    penalty = 0.2 * (1.0 - jnp.exp(ref_row - new_row))
    zero = jnp.zeros_like(weight)
    return jnp.stack([weight, ratio, penalty, tok_reward, tok_group, zero, zero, zero], axis=0)


def turn_kernel(pos, cot_a, cot_b, out_a, out_b):
    half, _ = out_a.shape
    rows = half // 8
    cols = pl.ds(pl.multiple_of(pos[0] * half, half), half)
    for cot, out in ((cot_a, out_a), (cot_b, out_b)):
        turned = cot[:, cols].astype(f32).T.astype(bf16)
        for y in range(4):
            out[y * rows : (y + 1) * rows, :] = turned[2 * y * rows : (2 * y + 1) * rows]
            to = pl.multiple_of((4 + (y - pos[3] + 4) % 4) * rows, rows)
            out[pl.ds(to, rows), :] = turned[(2 * y + 1) * rows : (2 * y + 2) * rows]


def turn(pos, cot_a, cot_b):
    toks, kv = cot_a.shape
    whole = lambda *shape: pl.BlockSpec(shape, lambda i, p: (0,) * len(shape))
    return pl.pallas_call(
        turn_kernel,
        out_shape=[jax.ShapeDtypeStruct((kv // 2, toks), bf16)] * 2,
        grid_spec=pltpu.PrefetchScalarGridSpec(
            num_scalar_prefetch=1,
            grid=(1,),
            in_specs=[whole(toks, kv)] * 2,
            out_specs=[whole(kv // 2, toks)] * 2,
        ),
        compiler_params=params(),
        cost_estimate=cost(4 * cot_a.size, 6 * cot_a.size),
        name="turn",
    )(pos, cot_a, cot_b)


def partial_kernel(pos, stats, tok_a, tok_b, cot_a, cot_b, hid_a, hid_b, *refs):
    outs, (hid, sems) = refs[:8], refs[8:]
    rows, blk = outs[0].shape[1:]
    copies = []
    for d in range(4):
        cols = pl.ds(pl.multiple_of((pos[1] + d) % 4 * blk, LANES), blk)
        for k, src in enumerate((hid_a, hid_b)):
            copies.append(pltpu.make_async_copy(src.at[:, cols], hid.at[d, k], sems.at[d, k]))
    for copy in copies:
        copy.start()
    sums = jnp.sum(stats[...], axis=0)
    count = jnp.maximum(sums[0:1, :], 1.0)
    mean = sums[1:2, :] / count
    spread = jnp.maximum(jnp.sqrt(jnp.maximum(sums[2:3, :] / count - mean * mean, 0.0)), 0.5)
    table = jnp.concatenate([jnp.broadcast_to(mean, (8, LANES)), jnp.broadcast_to(spread, (8, LANES))], axis=0).T
    mean, spread = table[:, 0:1], table[:, 8:9]
    delta = []
    for tok, cot in ((tok_a, cot_a), (tok_b, cot_b)):
        t = tok[...]
        group = lax.broadcasted_iota(jnp.int32, (LANES, t.shape[1]), 0).astype(f32)
        pick = group == t[4:5]
        tok_mean = jnp.sum(jnp.where(pick, mean, 0.0), axis=0, keepdims=True)
        tok_std = jnp.sum(jnp.where(pick, spread, 0.0), axis=0, keepdims=True)
        adv = (t[3:4] - tok_mean) / tok_std
        coef = t[0:1] * (-adv * t[1:2] + t[2:3])
        delta.append((cot[...].astype(f32) * coef).astype(bf16))
    for d in range(4):
        copies[2 * d].wait()
        acc = jnp.dot(delta[0], hid[d, 0], preferred_element_type=f32)
        copies[2 * d + 1].wait()
        acc = acc + jnp.dot(delta[1], hid[d, 1], preferred_element_type=f32)
        acc = acc.astype(bf16).reshape(8, rows, blk)
        outs[d][...] = acc[:4]
        for e in range(4):
            outs[4 + e][(pos[1] + d) % 4] = acc[4 + e]


def partial_product(pos, stats, tok_a, tok_b, cot_a, cot_b, hid_a, hid_b):
    toks, width = hid_a.shape
    half = cot_a.shape[0]
    blk = width // 4
    shape = (4, half // 8, blk)
    whole = lambda s: pl.BlockSpec(s, lambda i, p: (0,) * len(s))
    far = pl.BlockSpec(memory_space=pltpu.HBM)
    return pl.pallas_call(
        partial_kernel,
        out_shape=[jax.ShapeDtypeStruct(shape, bf16)] * 8,
        grid_spec=pltpu.PrefetchScalarGridSpec(
            num_scalar_prefetch=1,
            grid=(1,),
            in_specs=[whole(a.shape) for a in (stats, tok_a, tok_b, cot_a, cot_b)] + [far, far],
            out_specs=[whole(shape)] * 8,
            scratch_shapes=[pltpu.VMEM((4, 2, toks, blk), bf16), pltpu.SemaphoreType.DMA((4, 2))],
        ),
        compiler_params=params(50 * 1024 * 1024),
        cost_estimate=cost(4 * toks * width * half, 4 * toks * width + 2 * width * half),
        name="partial_product",
    )(pos, stats, tok_a, tok_b, cot_a, cot_b, hid_a, hid_b)


def sum_mid_kernel(axis, pos, *refs):
    srcs, outs = refs[:4], refs[4:]
    for d in range(4):
        k = (pos[axis] + d) % 4
        outs[d][...] = sum(src[k].astype(f32) for src in srcs).astype(bf16)


def sum_mid(pos, parts, axis):
    _, rows, width = parts[0].shape
    whole = lambda *shape: pl.BlockSpec(shape, lambda i, p: (0,) * len(shape))
    return pl.pallas_call(
        lambda *refs: sum_mid_kernel(axis, *refs),
        out_shape=[jax.ShapeDtypeStruct((rows, width), bf16)] * 4,
        grid_spec=pltpu.PrefetchScalarGridSpec(
            num_scalar_prefetch=1,
            grid=(1,),
            in_specs=[whole(4, rows, width)] * 4,
            out_specs=[whole(rows, width)] * 4,
        ),
        compiler_params=params(),
        cost_estimate=cost(16 * rows * width, 40 * rows * width),
    )(pos, *parts)


def sum_turn_kernel(*refs):
    srcs, out = refs[:8], refs[8]
    first = sum(src[...].astype(f32) for src in srcs[:4])
    second = sum(src[...].astype(f32) for src in srcs[4:])
    out[...] = jnp.concatenate([first, second], axis=0).T.astype(bf16)


def sum_turn(first, second):
    rows, width = first[0].shape
    return pl.pallas_call(
        sum_turn_kernel,
        out_shape=jax.ShapeDtypeStruct((width, 2 * rows), bf16),
        compiler_params=params(),
        cost_estimate=cost(8 * rows * width, 20 * rows * width),
        name="sum_turn",
    )(*first, *second)


def sum_spread_kernel(src, out):
    total = jnp.sum(src[...].astype(f32), axis=0).astype(bf16)
    for i in range(out.shape[0]):
        out[i] = total


def sum_spread(blocks, copies):
    n, rows, width = blocks.shape
    return pl.pallas_call(
        sum_spread_kernel,
        out_shape=jax.ShapeDtypeStruct((copies, rows, width), bf16),
        compiler_params=params(),
        cost_estimate=cost(n * rows * width, 4 * n * rows * width),
        name="sum_spread",
    )(blocks)


def send_kernel(pos, grad, blocks):
    g = grad[...].astype(f32)
    s = jnp.sum(g * g, axis=(0, 1, 2))
    s = jnp.sum(jnp.sum(s, axis=0, keepdims=True), axis=1, keepdims=True)
    high = s.astype(bf16).astype(f32)
    mid = (s - high).astype(bf16).astype(f32)
    low = s - high - mid
    rows = grad.shape[3]
    row = lax.broadcasted_iota(jnp.int32, (8, 2 * HEAD), 0)
    tail = jnp.where(row == 0, high, jnp.where(row == 1, mid, jnp.where(row == 2, low, 0.0))).astype(bf16)
    for h in range(KV_HEADS):
        for i in range(2):
            for j in range(2):
                for kv in range(2):
                    blocks[i, h, j, :rows, kv * HEAD : (kv + 1) * HEAD] = grad[pos[0], h, kv]
                blocks[i, h, j, rows:, :] = tail


def send_blocks(pos, grad):
    rows = grad.shape[3]
    whole = lambda s: pl.BlockSpec(s, lambda i, p: (0,) * len(s))
    shape = (2, KV_HEADS, 2, rows + 8, 2 * HEAD)
    return pl.pallas_call(
        send_kernel,
        out_shape=jax.ShapeDtypeStruct(shape, bf16),
        grid_spec=pltpu.PrefetchScalarGridSpec(
            num_scalar_prefetch=1, grid=(1,), in_specs=[whole(grad.shape)], out_specs=whole(shape)
        ),
        compiler_params=params(60 * 1024 * 1024),
        cost_estimate=cost(4 * grad.size, 8 * grad.size),
        name="send_blocks",
    )(pos, grad)


def step_size(squares, entries):
    s = jnp.sum(squares[...].astype(f32), axis=0)[:, 0:1]
    total = s[0:1] + s[1:2] + s[2:3]
    return 0.5 / jnp.sqrt(total / entries + 1e-06)


def update_kernel(entries, squares, grad, master, new):
    zl, ny, _, rows, width = grad.shape
    step = step_size(squares, entries)
    for kv in range(2):
        for y in range(ny):
            for z in range(zl):
                r = slice(z * rows, (z + 1) * rows)
                c = slice((kv * ny + y) * width, (kv * ny + y + 1) * width)
                new[r, c] = master[0, r, c] - grad[z, y, kv].astype(f32) * step


def update(received, grad, master, entries):
    _, rows, kv = master.shape
    return pl.pallas_call(
        lambda *refs: update_kernel(entries, *refs),
        out_shape=jax.ShapeDtypeStruct((rows, kv), f32),
        grid=(1,),
        in_specs=[
            pl.BlockSpec((received.shape[0], 8, LANES), lambda i: (0, rows // 16, 0)),
            pl.BlockSpec(grad.shape, lambda i: (0, 0, 0, 0, 0)),
            pl.BlockSpec((1, rows, kv), lambda i: (0, 0, 0)),
        ],
        out_specs=pl.BlockSpec((rows, kv), lambda i: (0, 0)),
        compiler_params=params(),
        cost_estimate=cost(4 * rows * kv, 10 * rows * kv),
        name="update",
    )(received, grad, master)


def rest_kernel(pos, *refs):
    masters, outs = refs[:8], refs[8:]
    for d in range(4):
        for kv in range(2):
            outs[d][0, :, :, kv * HEAD : (kv + 1) * HEAD] = masters[2 * d + kv][...].astype(bf16)


def rest_blocks(pos, master):
    layers, rows, kv = master.shape
    half = rows // 2

    def spec(d, k):
        return pl.BlockSpec(
            (layers, half, HEAD),
            lambda xl, p: (0, p[0], k * KV_HEADS + xl * 2 + ((p[2] + d) % 4) // 2),
        )

    shape = (2, layers, half, 2 * HEAD)
    return pl.pallas_call(
        rest_kernel,
        out_shape=[jax.ShapeDtypeStruct(shape, bf16)] * 4,
        grid_spec=pltpu.PrefetchScalarGridSpec(
            num_scalar_prefetch=1,
            grid=(2,),
            in_specs=[spec(d, k) for d in range(4) for k in range(2)],
            out_specs=[pl.BlockSpec((1, *shape[1:]), lambda xl, p: (xl, 0, 0, 0))] * 4,
        ),
        compiler_params=params(),
        cost_estimate=cost(layers * rows * kv, 12 * rows * kv),
        name="rest_blocks",
    )(pos, *([master] * 8))


def mark_kernel(src, out):
    out[...] = src[...]


def mark(value):
    return pl.pallas_call(
        mark_kernel,
        out_shape=jax.ShapeDtypeStruct(value.shape, value.dtype),
        compiler_params=params(),
        name="mark",
    )(value)


def regroup_kernel(pos, after, *refs):
    parts, outs, (held, sems, out_sems) = refs[:4], refs[4:6], refs[6:]
    xl = pos[1] % 2
    copies = []
    for d in range(4):
        for k, at in enumerate((xl, 1 - xl)):
            into = pltpu.make_async_copy(parts[d].at[at], held.at[d, k], sems.at[d, k])
            away = pltpu.make_async_copy(held.at[d, k], outs[k].at[d], out_sems.at[d, k])
            copies.append((into, away))
    for into, _ in copies:
        into.start()
    for into, away in copies:
        into.wait()
        away.start()
    for _, away in copies:
        away.wait()


def regroup(pos, parts, after):
    shape = (4, *parts[0].shape[1:])
    far = pl.BlockSpec(memory_space=pltpu.HBM)
    return pl.pallas_call(
        regroup_kernel,
        out_shape=[jax.ShapeDtypeStruct(shape, bf16)] * 2,
        grid_spec=pltpu.PrefetchScalarGridSpec(
            num_scalar_prefetch=1,
            grid=(1,),
            in_specs=[pl.BlockSpec(memory_space=pl.ANY)] + [far] * 4,
            out_specs=[far] * 2,
            scratch_shapes=[
                pltpu.VMEM((4, 2, *shape[1:]), bf16),
                pltpu.SemaphoreType.DMA((4, 2)),
                pltpu.SemaphoreType.DMA((4, 2)),
            ],
        ),
        compiler_params=params(),
        cost_estimate=cost(parts[0].size, 16 * parts[0].size),
        name="regroup",
    )(pos, after, *parts)


def place_rest_kernel(pos, *refs):
    srcs, out = refs[:8], refs[8]
    zh, core = pos[2], pos[0]
    for dx in range(4):

        @pl.when(pl.program_id(1) == dx)
        def _():
            for w in range(2):
                for dz in range(4):
                    out[0, 0, (zh - dz + 4) % 4, (core + w) % 2] = srcs[4 * w + dx][dz, 0]


def place_rest(pos, own, other, layers):
    _, count, half, width = own[0].shape
    src = pl.BlockSpec((4, 1, half, width), lambda l, d, p: (0, 1 + l, 0, 0))
    return pl.pallas_call(
        place_rest_kernel,
        out_shape=jax.ShapeDtypeStruct((layers, 4, 4, 2, half, width), bf16),
        grid_spec=pltpu.PrefetchScalarGridSpec(
            num_scalar_prefetch=1,
            grid=(count - 1, 4),
            in_specs=[src] * 8,
            out_specs=pl.BlockSpec(
                (1, 1, 4, 2, half, width), lambda l, d, p: (1 + l, (p[1] - d + 4) % 4, 0, 0, 0, 0)
            ),
        ),
        compiler_params=params(58 * 1024 * 1024),
        cost_estimate=cost(own[0].size, 32 * own[0].size),
        name="place_rest",
    )(pos, *own, *other)


def finish_kernel(entries, pos, squares, grad_a, grad_b, *refs):
    masters, out = refs[:8], refs[9]
    zh, core = pos[2], pos[0]
    step = step_size(squares, entries)
    half = out.shape[4]
    for dx in range(4):

        @pl.when(pl.program_id(0) == dx)
        def _():
            for w in range(2):
                grad = (grad_a, grad_b)[w]
                for dz in range(4):
                    k = (zh - dz + 4) % 4
                    value = masters[4 * w + dx][dz, 0].astype(f32) - grad[k, :half].astype(f32) * step
                    out[0, 0, k, (core + w) % 2] = value.astype(bf16)


def finish(pos, grad_a, grad_b, own, other, into, entries):
    n, padded, width = grad_a.shape
    half = padded - 8
    grad = pl.BlockSpec((4, padded, width), lambda d, p: ((p[1] - d + 4) % 4, 0, 0))
    src = pl.BlockSpec((4, 1, half, width), lambda d, p: (0, 0, 0, 0))
    return pl.pallas_call(
        lambda *refs: finish_kernel(entries, *refs),
        out_shape=jax.ShapeDtypeStruct(into.shape, bf16),
        grid_spec=pltpu.PrefetchScalarGridSpec(
            num_scalar_prefetch=1,
            grid=(4,),
            in_specs=[pl.BlockSpec((n, 8, LANES), lambda d, p: (0, half // 8, 0)), grad, grad]
            + [src] * 8
            + [pl.BlockSpec(memory_space=pl.ANY)],
            out_specs=pl.BlockSpec(
                (1, 1, 4, 2, half, width), lambda d, p: (0, (p[1] - d + 4) % 4, 0, 0, 0, 0)
            ),
        ),
        input_output_aliases={12: 0},
        compiler_params=params(),
        cost_estimate=cost(8 * grad_a.size, 24 * grad_a.size),
        name="finish",
    )(pos, grad_a, grad_a, grad_b, *own, *other, into)


def per_device(
    hidden,
    cotangent,
    seq_ids,
    response_mask,
    group_ids,
    rewards,
    new_logp,
    old_logp,
    ref_logp,
    master,
):
    n_y, n_z = lax.axis_size("y"), lax.axis_size(("zh", "zl"))
    n_shard = lax.axis_size(SHARD)
    layers, rows, kv = master.shape
    pos = jnp.stack([lax.axis_index(a).astype(jnp.int32) for a in ("c", "x", "zh", "y")])

    first, second = ("x", "y"), ("zh", "zl", "c")
    stats = exchanged(group_sums(group_ids, rewards, lax.axis_size(first)), first)
    stats = stats_spread(stats, lax.axis_size(second))
    stats = exchanged(stats, second)

    hidden_b = swapped(hidden)
    cotangent_b = swapped(cotangent)
    tok = token_rows(
        seq_ids[0], response_mask[0], group_ids[0], rewards[0], new_logp[0], old_logp[0], ref_logp[0]
    )
    tok_b = swapped(tok)

    turned = turn(pos, cotangent, cotangent_b)
    partial = partial_product(pos, stats, tok, tok_b, *turned, hidden, hidden_b)
    to_x = spread_out(partial[:4], "x")
    to_y = spread_out(partial[4:], "y")
    to_x = sum_mid(pos, to_x, 3)
    to_x = spread_out(to_x, "y")
    to_y = sum_mid(pos, to_y, 1)
    to_y = spread_out(to_y, "x")
    part = sum_turn(to_x, to_y)

    parts = rest_blocks(pos, master)
    parts = spread_out(parts, "zh")
    same, cross = regroup(pos, parts, mark(rewards))
    rest = spread_out([same, cross, same, cross], "x")
    part = part.reshape(n_z, part.shape[0] // n_z, part.shape[1])
    zl = lax.axis_size("zl")
    part = exchanged(part, ("zh", "zl"))
    grad = exchanged(sum_spread(part, zl * n_y * 2), REP)
    grad = grad.reshape(zl, n_y, 2, *grad.shape[1:])
    first = send_blocks(pos, grad)
    first = exchanged(first.reshape(n_shard, *first.shape[3:]), SHARD)

    other = [swapped(r) for r in rest]
    out = place_rest(pos, rest, other, layers)
    entries = hidden.shape[1] * kv
    first_b = swapped(first)
    new_master = update(first, grad, master, entries)
    out = finish(pos, first, first_b, rest, other, out, entries)
    return (new_master, out.reshape(layers, n_shard * rows, 2 * HEAD))


def solution(mesh):
    split = Mesh(mesh.devices.reshape(2, 4, 2, 4, 4), REP + SHARD)
    row = P(REP + SHARD, None)
    return jax.shard_map(
        per_device,
        mesh=split,
        in_specs=(row,) * 9 + (P(None, SHARD, None),),
        out_specs=(P(SHARD, None), P(None, None, SHARD)),
        check_vma=False,
    )
```
